32 devices in a mesh: tracts: 2 (over y), sky: 4 (over z), depth: 4 (over x, core).
Axes of the slice: x: 2, y: 2, z: 4, core: 2. Of those that a mesh axis runs over, the one named last changes fastest.
Arguments:
- visit_tiles: bfloat16 [128, 4, 64, 512], P(('tracts', 'sky', 'depth')), parts along dimension 0, may hold values from -6 to 6
- warp_matrix: bfloat16 [128, 512, 512], P(('tracts', 'sky', 'depth')), parts along dimension 0, may hold values from -0.25 to 0.25
- flux_scale: float32 [128], P(('tracts', 'sky', 'depth')), parts along dimension 0, may hold values from 0.3 to 3
- patch_lists: int32 [128, 4], P(('tracts', 'sky', 'depth')), parts along dimension 0, may hold values from 0 to 15, all different within a row; in each aligned block of 4 rows (0 to 3, 4 to 7, ...) at most 2 rows name the same one
- clip_bits: int32 [128, 4, 4, 512], P(('tracts', 'sky', 'depth')), parts along dimension 0, may hold values from -2147483648 to 2147483647, as said below
Outputs:
- coadd_mean: float32 [2, 32, 64, 512], P(None, ('tracts', 'sky'), 'depth'), parts along dimension 1
- coadd_var: float32 [2, 32, 64, 512], P(None, ('tracts', 'sky'), 'depth'), parts along dimension 1
The draws below stay inside these ranges and needn't reach their ends.
There are 2 independent parts, one for each index of `tracts`. The reference program is written for one: setup_inputs(seed, part) draws one part's arguments, and reference() takes and returns one part's arrays. A program takes and returns all parts, laid end to end along the dimension named above; each array names one. Nothing has to cross between parts.
Inputs may be any that keep to these rules, and one draw needn't show every extreme that they name: `patch_lists`: row v names the 4 different patches of visit v's blocks. In the rows of one device no patch is named more than 2 times, a bound that some block reaches there; every patch is named by some row. Bit 16 t + j of clip_bits[v, k, g, c] is 1 when clip pass t (t = 0 or 1) keeps the sample of visit v's block k at row 16 g + j, column c.
All inputs are finite; a program needn't handle non-finite values.
Results may differ from the reference program's by a relative error of at most 0.0029.
Values may be sent and summed in bfloat16 or wider, within the bound.
A program may use at most 128 MiB of HBM per device.

```python
import math
import jax
import jax.numpy as jnp
import numpy as np
from jax import lax

COLUMNS = 512
ROWS = 64
VISITS_DEV = 4
CAPACITY = 2
PATCHES = 16
INTERSECTIONS = 4
VISITS = 64


def draw_clip_bits(key, part):
    word_shape = (VISITS, INTERSECTIONS, ROWS // 16, COLUMNS)

    def add_bit(position, packed):
        level = jax.random.randint(jax.random.fold_in(key, position + 7), word_shape, 0, 20, dtype=jnp.int32)
        limit = jnp.where(position < 16, 18, 17)
        kept = (level < limit).astype(jnp.int32)
        return jnp.bitwise_or(packed, jnp.left_shift(kept, position))
    return lax.fori_loop(0, 32, add_bit, jnp.zeros(word_shape, jnp.int32))


def levels(own_key, dims, shards, low, top_value):
    loudness = 1.0
    for dim, parts in shards:
        heights = jax.random.uniform(jax.random.fold_in(jax.random.fold_in(own_key, 6), dim), (parts,), jnp.float32, low / len(shards), top_value / len(shards))
        loudness = loudness * jnp.repeat(jnp.exp(heights), dims[dim] // parts).reshape((-1,) + (1,) * (len(dims) - 1 - dim))
    return loudness


def routed_block(rng, own, number, rows, amount, top, most, lean):
    sequence = jax.random.permutation(rng, amount)
    crowded, common = load_shares(amount, rows * top, most, lean, True), load_shares(amount, rows * top, most, lean, False)
    places = jnp.arange(amount)

    def named(tallies, turn):
        used = int((tallies > 0).sum())
        fixed = max(1, used // 4)
        passed = fixed + (places - fixed + turn * (used - fixed)) % max(1, amount - fixed)
        return jnp.zeros((amount,), jnp.int32).at[sequence[jnp.where(places < fixed, places, passed)]].set(jnp.asarray(tallies, jnp.int32))

    tallies = jnp.where(number % 4 == 0, named(crowded, number // 4), named(common, number - number // 4 - 1))
    mixed = jax.random.permutation(jax.random.fold_in(own, 3), amount)
    giver, receiver = mixed[0:amount // 2 * 2:2], mixed[1:amount // 2 * 2:2]
    room = jnp.minimum(tallies[giver] - 1, most - tallies[receiver]) // 2
    room = jnp.where((giver == sequence[0]) | (receiver == sequence[0]) | (tallies[receiver] == 0), 0, jnp.maximum(room, 0))
    passed = jax.random.randint(jax.random.fold_in(own, 4), (amount // 2,), 0, 1 << 20) % (room + 1)
    tallies = tallies.at[giver].add(-passed).at[receiver].add(passed)
    members = jnp.searchsorted(jnp.cumsum(tallies), jnp.arange(rows * top), side="right").astype(jnp.int32)
    listing = members.reshape(top, rows).T
    listing = listing[jax.random.permutation(jax.random.fold_in(own, 1), rows)]
    turn = jax.random.randint(jax.random.fold_in(own, 2), (rows, 1), 0, top)
    return jnp.take_along_axis(listing, (jnp.arange(top)[None, :] + turn) % top, axis=1)


def load_shares(count, total, most, lean, full):
    weights = [(1 << 20) // math.isqrt(grade ** lean) + 1 for grade in range(1, count + 1)]
    largest = most if full else min(most, max(-(-total // count), total * weights[0] // sum(weights)))
    least = 1 if total - largest >= count - 1 else 0
    counts, surplus = [largest] + [least] * (count - 1), total - largest - least * (count - 1)
    while surplus > 0:
        candidates = [i for i in range(1, count) if counts[i] < largest] or [i for i in range(1, count) if counts[i] < most]
        mass, remaining = sum([weights[i] for i in candidates]), surplus
        for i in candidates:
            extra = min(most - counts[i], max(1, remaining * weights[i] // mass), surplus)
            counts[i] = counts[i] + extra
            surplus = surplus - extra
    return np.array(counts)


def scatter_about(rng, extent, deviation, reach, cuts=(), held_as=jnp.bfloat16):
    entries = jax.random.normal(rng, extent, jnp.float32) * deviation
    if len(cuts) > 0:
        entries = levels(rng, extent, cuts, -0.22, 0.18) * entries
    return jnp.clip(entries, min=-reach, max=reach).astype(held_as)


def setup_inputs(seed: int = 0, part: int = 0) -> dict:
    key_list = jax.random.split(jax.random.key(seed), 6)
    part_splits = jax.random.split(jax.random.fold_in(key_list[5], part), 6)
    visit_tiles = scatter_about(part_splits[0], (VISITS, INTERSECTIONS, ROWS, COLUMNS), 1.0, 6.0, ((0, 16),))
    warp_matrix = scatter_about(part_splits[1], (VISITS, COLUMNS, COLUMNS), COLUMNS ** -0.5, 0.25, ((0, 16),))
    flux_scale = jnp.clip(jnp.exp(math.log(3.0) - 2.3025851 * jax.random.uniform(part_splits[2], (VISITS,), jnp.float32) ** levels(part_splits[2], (VISITS,), ((0, 16),), -0.2, 0.2)), 0.3, 3.0)
    patch_lists_keys = jax.random.split(jax.random.fold_in(part_splits[3], 1), VISITS // VISITS_DEV)
    patch_lists_turns = jax.random.permutation(jax.random.fold_in(part_splits[3], 3), VISITS // VISITS_DEV)
    patch_lists = jax.vmap(lambda own, number: routed_block(jax.random.fold_in(part_splits[3], 2), own, number, VISITS_DEV, PATCHES, INTERSECTIONS, CAPACITY, 2))(patch_lists_keys, patch_lists_turns).reshape((VISITS, INTERSECTIONS))
    clip_bits = draw_clip_bits(jax.random.fold_in(jax.random.fold_in(key_list[5], part), 71), part)
    return {"visit_tiles": visit_tiles, "warp_matrix": warp_matrix, "flux_scale": flux_scale, "patch_lists": patch_lists, "clip_bits": clip_bits}


def unpack_keep(packed, offset):
    positions = jnp.arange(16, dtype=jnp.int32) + offset
    bit_flags = jnp.bitwise_and(jnp.right_shift(packed[..., None, :], positions[:, None]), 1)
    target_shape = packed.shape[:-2] + (packed.shape[-2] * 16, packed.shape[-1])
    return bit_flags.reshape(target_shape).astype(jnp.float32)


def finish(count_first, sum_first, square_first, count_both, shift_sum, shift_square):
    first_mean = sum_first / jnp.maximum(count_first, 1.0)
    first_var = (square_first - sum_first * first_mean) / jnp.maximum(count_first - 1.0, 1.0)
    final_mean = first_mean + shift_sum / jnp.maximum(count_both, 1.0)
    final_var = (shift_square - shift_sum * shift_sum / jnp.maximum(count_both, 1.0)) / jnp.maximum(count_both - 1.0, 1.0)
    return jnp.stack([first_mean, final_mean]), jnp.stack([first_var, final_var])


def reference(visit_tiles, warp_matrix, flux_scale, patch_lists, clip_bits):
    def warp_one(member):
        tile_block, matrix, factor = member
        product = jnp.dot(tile_block.reshape(INTERSECTIONS * ROWS, COLUMNS), matrix, preferred_element_type=jnp.float32)
        return (product * factor).astype(jnp.bfloat16).reshape(INTERSECTIONS, ROWS, COLUMNS)

    warped = lax.map(warp_one, (visit_tiles, warp_matrix, flux_scale))
    initial = jnp.zeros((PATCHES, ROWS, COLUMNS), jnp.float32)

    def first_step(state_sums, member):
        counted, totals, squares = state_sums
        warped_rows, packed, targets = member
        samples = warped_rows.astype(jnp.float32)
        keep_mask = unpack_keep(packed, 0)
        return (counted.at[targets].add(keep_mask), totals.at[targets].add(keep_mask * samples),
                squares.at[targets].add(keep_mask * samples * samples)), None

    (count_first, sum_first, square_first), _ = lax.scan(first_step, (initial, initial, initial), (warped, clip_bits, patch_lists))
    first_mean = sum_first / jnp.maximum(count_first, 1.0)

    def second_step(state_sums, member):
        counted, totals, squares = state_sums
        warped_rows, packed, targets = member
        samples = warped_rows.astype(jnp.float32)
        keep_mask = unpack_keep(packed, 0) * unpack_keep(packed, 16)
        centred = samples - first_mean[targets]
        return (counted.at[targets].add(keep_mask), totals.at[targets].add(keep_mask * centred),
                squares.at[targets].add(keep_mask * centred * centred)), None

    (count_both, shift_sum, shift_square), _ = lax.scan(second_step, (initial, initial, initial), (warped, clip_bits, patch_lists))
    return finish(count_first, sum_first, square_first, count_both, shift_sum, shift_square)
```

```python
import functools

import jax
import jax.numpy as jnp
from jax import lax
from jax.experimental import pallas as pl
from jax.experimental.pallas import tpu as pltpu
from jax.sharding import PartitionSpec as P

PATCH_DEV = 4
CAPACITY = 2
SLOTS = PATCH_DEV * CAPACITY
MESH = pl.DeviceIdType.MESH
STEP = 4
LAG = 3
LEAD = 2


def kernel(sky, depth, scale_ref, src_ref, tiles_ref, matrix_ref, bits_ref, mean_ref, var_ref,
           warped, send_t, send_b, recv_t, recv_b, acc, st, sb, rt, rb):
    z, d = lax.axis_index("sky"), lax.axis_index("depth")
    me = z * depth + d
    devices = sky * depth
    visits, entries_rows, columns = tiles_ref.shape
    entries, rows, _ = warped.shape
    share = rows // depth

    def place(j):
        return lax.div(lax.rem(me + j, devices), depth), lax.rem(lax.rem(me + j, devices), depth)

    barrier = pltpu.get_barrier_semaphore()

    def greet(j, _):
        zz, dd = place(j)
        pl.semaphore_signal(barrier, inc=1, device_id={"sky": zz, "depth": dd}, device_id_type=MESH)
        return 0

    lax.fori_loop(1, devices, greet, 0)

    per_visit = entries // visits
    for v in range(visits):
        def warp(i, _, v=v):
            start = pl.multiple_of(i * STEP * rows, STEP * rows)
            product = jnp.dot(tiles_ref[v, pl.ds(start, STEP * rows), :], matrix_ref[v],
                              preferred_element_type=jnp.float32) * scale_ref[v]
            warped[pl.ds(v * per_visit + i * STEP, STEP)] = product.astype(jnp.bfloat16).reshape(STEP, rows, columns)
            return 0
        lax.fori_loop(0, per_visit // STEP, warp, 0)

    pl.semaphore_wait(barrier, devices - 1)

    def copies(zz, dd, there, mine):
        to = {"sky": zz, "depth": dd}
        return (
            pltpu.make_async_remote_copy(src_ref=send_t.at[there], dst_ref=recv_t.at[mine], send_sem=st.at[there],
                                         recv_sem=rt.at[mine], device_id=to, device_id_type=MESH),
            pltpu.make_async_remote_copy(src_ref=send_b.at[there], dst_ref=recv_b.at[mine], send_sem=sb.at[there],
                                         recv_sem=rb.at[mine], device_id=to, device_id_type=MESH),
        )

    def post(jj, _):
        zz = lax.rem(z + sky // 2 + jj, sky)

        def fill(s, _):
            e = src_ref[zz * SLOTS + s]
            valid = (e < entries).astype(jnp.int32)
            e = jnp.minimum(e, entries - 1)
            block = warped[e]
            flags = bits_ref[e] * valid
            for dd in range(depth):
                send_t[zz * depth + dd, s] = block[dd * share:(dd + 1) * share]
                send_b[zz * depth + dd, s] = flags[dd * (share // 16):(dd + 1) * (share // 16)]
            return 0

        lax.fori_loop(0, SLOTS, fill, 0)

        def start(k, _):
            dd = lax.rem(d + k, depth)
            there = zz * depth + dd

            @pl.when(there != me)
            def _():
                for c in copies(zz, dd, there, me):
                    c.start()
            return 0

        lax.fori_loop(0, depth, start, 0)
        return 0

    lax.fori_loop(0, sky, post, 0)

    acc[...] = jnp.zeros_like(acc)
    position = lax.rem(lax.broadcasted_iota(jnp.int32, (share, columns), 0), 16)

    def add(tiles, flags, source):
        for p in range(PATCH_DEV):
            sums = [acc[p, q] for q in range(6)]
            for c in range(CAPACITY):
                w = tiles[source, p * CAPACITY + c].astype(jnp.float32)
                packed = flags[source, p * CAPACITY + c]
                packed = jnp.broadcast_to(packed[:, None, :], (share // 16, 16, columns)).reshape(share, columns)
                shifted = lax.shift_right_logical(packed, position)
                first = (shifted & 1).astype(jnp.float32)
                both = first * (lax.shift_right_logical(shifted, 16) & 1).astype(jnp.float32)
                fw, bw = first * w, both * w
                for q, term in enumerate((first, fw, fw * w, both, bw, bw * w)):
                    sums[q] = sums[q] + term
            for q in range(6):
                acc[p, q] = sums[q]

    add(send_t, send_b, me)

    def take(jj, _):
        zz = lax.rem(z - sky // 2 - jj + 2 * sky, sky)

        def one(k, _):
            dd = lax.rem(d - k + depth, depth)
            there = zz * depth + dd

            @pl.when(there != me)
            def _():
                for c in copies(zz, dd, there, there):
                    c.wait_recv()
                add(recv_t, recv_b, there)
            return 0

        lax.fori_loop(0, depth, one, 0)
        return 0

    lax.fori_loop(0, sky, take, 0)

    for p in range(PATCH_DEV):
        cf, sf, qf, cb, sb_, qb = [acc[p, q] for q in range(6)]
        mean = sf / jnp.maximum(cf, 1.0)
        shift = sb_ - mean * cb
        square = qb - mean * sb_ - mean * shift
        step = shift / jnp.maximum(cb, 1.0)
        mean_ref[0, p] = mean
        mean_ref[1, p] = mean + step
        var_ref[0, p] = (qf - sf * mean) / jnp.maximum(cf - 1.0, 1.0)
        var_ref[1, p] = (square - shift * step) / jnp.maximum(cb - 1.0, 1.0)

    def drain(j, _):
        zz, dd = place(j)
        for c in copies(zz, dd, zz * depth + dd, me):
            c.wait_send()
        return 0

    lax.fori_loop(1, devices, drain, 0)


def folded(depth, scale_hbm, lists_hbm, tiles_hbm, matrix_hbm, bits_hbm, out_ref,
           scale_ref, lists_ref, tiles_ref, matrix_ref, bits_ref, s_in,
           out_t, out_b, row_t, row_b, raw_t, raw_b, own_s, row_s, raw_s, far32, far16, got32, got16, tables, local,
           work_t, work_b,
           s_xt, r_xt, s_xb, r_xb, s_xs, r_xs, s_ms, r_ms, s_dt, r_dt, s_db, r_db, s_ft, r_ft, s_fb, r_fb,
           s_f, r_f, s_h, r_h, s_l):
    z, d = lax.axis_index("sky"), lax.axis_index("depth")
    half = z // 2
    rem = z - 2 * half
    inner, outer = rem != half, rem == half
    mate = 2 * half + 1 - rem
    across, beyond = 3 - z, 3 - mate
    base = d // 2 * 2
    other = depth - 2 - base
    parts, _, entries, slab, width = out_t.shape
    groups_here = out_b.shape[0] * width // tiles_ref.shape[2]
    visits, entries_rows, columns = tiles_ref.shape
    per_visit = entries // visits
    rows = entries_rows // per_visit
    share = rows // depth
    slabs = share // slab
    long = own_s.shape[1]

    bands = matrix_ref.shape[0]
    tiles_in = pltpu.make_async_copy(tiles_hbm, tiles_ref, s_in.at[bands])
    bits_in = pltpu.make_async_copy(bits_hbm, bits_ref, s_in.at[bands + 1])
    scale_in = pltpu.make_async_copy(scale_hbm, scale_ref, s_in.at[bands + 2])
    lists_in = pltpu.make_async_copy(lists_hbm, lists_ref, s_in.at[bands + 3])

    def matrix_in(band):
        lanes = pl.ds(band * width, width)
        return pltpu.make_async_copy(matrix_hbm.at[:, :, lanes], matrix_ref.at[band], s_in.at[band])

    barrier = pltpu.get_barrier_semaphore()
    for k in range(1, depth):
        pl.semaphore_signal(barrier, inc=1, device_id={"depth": lax.rem(d + k, depth)}, device_id_type=MESH)
    for k in range(depth):
        pl.semaphore_signal(barrier, inc=1, device_id={"sky": mate, "depth": k}, device_id_type=MESH)
    pl.semaphore_signal(barrier, inc=1, device_id={"sky": beyond}, device_id_type=MESH)

    @pl.when(inner)
    def _():
        pl.semaphore_signal(barrier, inc=1, device_id={"sky": across}, device_id_type=MESH)

    tiles_in.start()
    matrix_in(0).start()
    lists_in.start()
    scale_in.start()
    bits_in.start()
    for band in range(1, bands):
        matrix_in(band).start()

    def remote(src, dst, send, recv, to):
        return pltpu.make_async_remote_copy(src_ref=src, dst_ref=dst, send_sem=send, recv_sem=recv, device_id=to,
                                            device_id_type=MESH)

    def to_row(c, there, slot):
        to = {"depth": there}
        return remote(out_t.at[c, there], row_t.at[c, slot], s_xt.at[c, there], r_xt.at[c, slot], to)

    def flags_to_row(b, there, slot):
        to = {"depth": there}
        return remote(out_b.at[b, there], row_b.at[b, slot], s_xb.at[b, there], r_xb.at[b, slot], to)

    def table_to_row(there, slot):
        return remote(own_s, row_s.at[slot], s_xs.at[there], r_xs.at[slot], {"depth": there})

    def table_to_mates(there, slot):
        return remote(own_s, raw_s.at[slot], s_ms.at[there], r_ms.at[slot], {"sky": mate, "depth": there})

    def direct(c, there, slot):
        to = {"sky": mate, "depth": there}
        return remote(out_t.at[c, there], raw_t.at[c, slot], s_dt.at[c, there], r_dt.at[c, slot], to)

    def flags_direct(b, there, slot):
        to = {"sky": mate, "depth": there}
        return remote(out_b.at[b, there], raw_b.at[b, slot], s_db.at[b, there], r_db.at[b, slot], to)

    def onward(c, start):
        pair = pl.ds(start, 2)
        return remote(row_t.at[c, pair], raw_t.at[c, pair], s_ft.at[c], r_ft.at[c], {"sky": mate})

    def flags_onward(b, start):
        pair = pl.ds(start, 2)
        return remote(row_b.at[b, pair], raw_b.at[b, pair], s_fb.at[b], r_fb.at[b], {"sky": mate})

    def sums_to(c, t, where, slot):
        to = {"sky": where}
        return (remote(far32.at[c, t], got32.at[c, slot], s_f.at[c, t], r_f.at[c, slot], to),
                remote(far16.at[c, t], got16.at[c, slot], s_h.at[c, t], r_h.at[c, slot], to))

    position = lax.broadcasted_iota(jnp.int32, (slab, width), 0)
    for which in range(2):
        for dd in range(depth):
            work_t[which, dd, entries] = jnp.zeros((slab, width), jnp.bfloat16)
            work_b[which, dd, entries] = jnp.zeros((1, width), jnp.int32)

    lists_in.wait()
    lane = lax.broadcasted_iota(jnp.int32, (1, long), 1)
    table = jnp.full((1, long), entries, jnp.int32)
    targets = [lists_ref[v, k] for v in range(visits) for k in range(per_visit)]
    for e in range(entries):
        rank = jnp.int32(0)
        for f in range(e // per_visit * per_visit):
            rank = rank + (targets[e] == targets[f]).astype(jnp.int32)
        table = jnp.where(lane == targets[e] * CAPACITY + rank, e, table)
    own_s[...] = table
    row_s[d] = table

    def stage(c, which, tiles, flags):
        work_t[which, :, :entries] = tiles[c]
        work_b[which, :, :entries] = flags[c // 2]

    def gather(c, patch, groups):
        place = position + (c % 2) * slab
        sums = [jnp.zeros((slab, width), jnp.float32)] * 6
        for which in range(groups):
            for dd in range(depth):
                for k in range(CAPACITY):
                    e = tables[which, dd, 0, patch * CAPACITY + k]
                    w = work_t[which, dd, e].astype(jnp.float32)
                    packed = jnp.broadcast_to(work_b[which, dd, e], (slab, width))
                    shifted = lax.shift_right_logical(packed, place)
                    first = (shifted & 1).astype(jnp.float32)
                    both = first * (lax.shift_right_logical(shifted, 16) & 1).astype(jnp.float32)
                    fw, bw = first * w, both * w
                    sums = [a + b for a, b in zip(sums, (first, fw, fw * w, both, bw, bw * w))]
        return sums

    def send_sums(c, t, where, groups):
        def one(p, _):
            cf, sf, qf, cb, sb, qb = gather(c, where * PATCH_DEV + p, groups)
            mean = sf / jnp.maximum(cf, 1.0)
            far32[c, t, p] = sf
            packed = (cf, cb, qf - sf * mean, sb - mean * cb, qb - sb * (sb / jnp.maximum(cb, 1.0)))
            for q, value in enumerate(packed):
                far16[c, t, p, q] = value.astype(jnp.bfloat16)
            return 0
        lax.fori_loop(0, PATCH_DEV, one, 0)
        for copy in sums_to(c, t, where, half):
            copy.start()

    def send_direct(c):
        @pl.when(c % 2 == 0)
        def _():
            for j in range(2):
                flags_direct(c // 2, base + j, d).start()
        for j in range(2):
            direct(c, base + j, d).start()

    def warp(column, _):
        lanes = pl.ds(pl.multiple_of(column * width, width), width)
        for band in range(bands):
            @pl.when(column == band)
            def _(band=band):
                matrix_in(band).wait()
        for v in range(visits):
            product = jnp.dot(tiles_ref[v], matrix_ref[column, v], preferred_element_type=jnp.float32)
            block = (product * scale_ref[v]).reshape(per_visit, depth, slabs, slab, width)
            for dd in range(depth):
                for h in range(slabs):
                    out_t[column * slabs + h, dd, v * per_visit:(v + 1) * per_visit] = block[:, dd, h].astype(jnp.bfloat16)
        for g in range(groups_here):
            b = column * groups_here + g
            for dd in range(depth):
                line = dd * groups_here + g
                out_b[b, dd] = bits_ref[:, line:line + 1, lanes]
            row_b[b, d] = out_b[b, d]
        for h in range(slabs):
            row_t[column * slabs + h, d] = out_t[column * slabs + h, d]

        @pl.when(column == 0)
        def _():
            @pl.when(inner)
            def _():
                pl.semaphore_wait(barrier, 2 * depth + 1)

            @pl.when(outer)
            def _():
                pl.semaphore_wait(barrier, 2 * depth)
            for k in range(1, depth):
                table_to_row(lax.rem(d + k, depth), d).start()

            @pl.when(outer)
            def _():
                for k in range(depth):
                    table_to_mates(k, d).start()

        for h in range(slabs):
            for k in range(1, depth):
                there = lax.rem(d + k, depth)
                if h % 2 == 0:
                    flags_to_row(column * groups_here + h // 2, there, d).start()
                to_row(column * slabs + h, there, d).start()

            @pl.when(jnp.logical_and(outer, column * slabs + h < LEAD))
            def _(h=h):
                send_direct(column * slabs + h)
        return 0

    tiles_in.wait()
    scale_in.wait()
    bits_in.wait()
    lax.fori_loop(0, bands, warp, 0)
    mine, theirs = (row_t, row_b), (raw_t, raw_b)

    for k in range(1, depth):
        table_to_row(lax.rem(d + k, depth), lax.rem(d + depth - k, depth)).wait_recv()
    held = pltpu.make_async_copy(row_s, tables.at[0], s_l.at[0])
    held.start()
    held.wait()

    def total(c, slot, p):
        sf = got32[c, slot, p]
        cf, cb, mf, shift, mb = [got16[c, slot, p, q].astype(jnp.float32) for q in range(5)]
        mean = sf / jnp.maximum(cf, 1.0)
        sb = shift + mean * cb
        return cf, sf, mf + sf * mean, cb, sb, mb + sb * (sb / jnp.maximum(cb, 1.0))

    def finish(c):
        lanes = pl.ds(pl.multiple_of(c // slabs * width, width), width)
        lines = pl.ds(pl.multiple_of(c % slabs * slab, slab), slab)
        stage(c, 0, *mine)

        @pl.when(inner)
        def _():
            stage(c, 1, *theirs)

            def one(p, _):
                for q, value in enumerate(gather(c, z * PATCH_DEV + p, 2)):
                    local[p, q] = value
                return 0
            lax.fori_loop(0, PATCH_DEV, one, 0)

        @pl.when(outer)
        def _():
            def one(p, _):
                for q, value in enumerate(gather(c, z * PATCH_DEV + p, 1)):
                    local[p, q] = value
                return 0
            lax.fori_loop(0, PATCH_DEV, one, 0)
            for copy in sums_to(c, 2, mate, half):
                copy.wait_recv()
            for p in range(PATCH_DEV):
                for q, value in enumerate(total(c, half, p)):
                    local[p, q] = local[p, q] + value

        for copy in sums_to(c, 0, across, 1 - half):
            copy.wait_recv()
        for p in range(PATCH_DEV):
            cf, sf, qf, cb, sb, qb = [local[p, q] + value for q, value in enumerate(total(c, 1 - half, p))]
            mean = sf / jnp.maximum(cf, 1.0)
            shift = sb - mean * cb
            square = qb - mean * sb - mean * shift
            step = shift / jnp.maximum(cb, 1.0)
            out_ref[0, 0, p, lines, lanes] = mean
            out_ref[0, 1, p, lines, lanes] = mean + step
            out_ref[1, 0, p, lines, lanes] = (qf - sf * mean) / jnp.maximum(cf - 1.0, 1.0)
            out_ref[1, 1, p, lines, lanes] = (square - shift * step) / jnp.maximum(cb - 1.0, 1.0)

    def forward(c, _):
        fresh = c % 2 == 0
        b = c // 2

        @pl.when(fresh)
        def _():
            for k in range(1, depth):
                flags_to_row(b, lax.rem(d + k, depth), lax.rem(d + depth - k, depth)).wait_recv()

        for k in range(1, depth):
            to_row(c, lax.rem(d + k, depth), lax.rem(d + depth - k, depth)).wait_recv()

        @pl.when(outer)
        def _():
            @pl.when(fresh)
            def _():
                flags_onward(b, other).start()
            onward(c, other).start()

            @pl.when(c + LEAD < parts)
            def _():
                send_direct(c + LEAD)

        @pl.when(inner)
        def _():
            stage(c, 0, *mine)
            send_sums(c, 2, mate, 1)

            @pl.when(c == 0)
            def _():
                for k in range(depth):
                    table_to_mates(k, k).wait_recv()
                more = pltpu.make_async_copy(raw_s, tables.at[1], s_l.at[1])
                more.start()
                more.wait()

            @pl.when(fresh)
            def _():
                for j in range(2):
                    flags_direct(b, base + j, base + j).wait_recv()
                flags_onward(b, other).wait_recv()

            for j in range(2):
                direct(c, base + j, base + j).wait_recv()
            onward(c, other).wait_recv()
            stage(c, 1, *theirs)
            send_sums(c, 0, beyond, 2)
            send_sums(c, 1, across, 2)

            @pl.when(c >= LAG)
            def _():
                finish(c - LAG)
        return 0

    lax.fori_loop(0, parts, forward, 0)

    def close(c, _):
        @pl.when(jnp.logical_or(outer, c >= parts - LAG))
        def _():
            finish(c)
        return 0

    lax.fori_loop(0, parts, close, 0)

    for k in range(1, depth):
        table_to_row(lax.rem(d + k, depth), d).wait_send()

    @pl.when(outer)
    def _():
        for k in range(depth):
            table_to_mates(k, d).wait_send()

    def drain_flags(b, _):
        for k in range(1, depth):
            flags_to_row(b, lax.rem(d + k, depth), d).wait_send()

        @pl.when(outer)
        def _():
            for j in range(2):
                flags_direct(b, base + j, d).wait_send()
            flags_onward(b, other).wait_send()
        return 0

    lax.fori_loop(0, parts // 2, drain_flags, 0)

    def drain(c, _):
        for k in range(1, depth):
            to_row(c, lax.rem(d + k, depth), d).wait_send()

        @pl.when(outer)
        def _():
            for j in range(2):
                direct(c, base + j, d).wait_send()
            onward(c, other).wait_send()

        @pl.when(inner)
        def _():
            for t, where in ((0, beyond), (1, across), (2, mate)):
                for copy in sums_to(c, t, where, half):
                    copy.wait_send()
        return 0

    lax.fori_loop(0, parts, drain, 0)


def split(both_ref, mean_hbm, var_hbm, sems):
    copies = [pltpu.make_async_copy(both_ref.at[q], out, sems.at[q]) for q, out in enumerate((mean_hbm, var_hbm))]
    for copy in copies:
        copy.start()
    for copy in copies:
        copy.wait()


def per_device(sky, depth, visit_tiles, warp_matrix, flux_scale, patch_lists, clip_bits):
    visits, own, rows, columns = visit_tiles.shape
    entries = visits * own
    patches = PATCH_DEV * sky
    devices = sky * depth
    share = rows // depth
    smem, vmem = pl.BlockSpec(memory_space=pltpu.SMEM), pl.BlockSpec(memory_space=pltpu.VMEM)
    hbm = pl.BlockSpec(memory_space=pltpu.HBM)
    out = jax.ShapeDtypeStruct((2, PATCH_DEV, share, columns), jnp.float32)
    if sky == 4 and depth == 4:
        width = 128
        slab = 8
        bands = columns // width
        parts = bands * (share // slab)
        long = -(-patches * CAPACITY // 128) * 128
        blocks = (parts, depth, entries, slab, width)
        flags = (parts // 2, depth, entries, 1, width)
        work = (2, depth, entries + 1)
        dma = pltpu.SemaphoreType.DMA
        both = pl.pallas_call(
            functools.partial(folded, depth),
            out_shape=jax.ShapeDtypeStruct((2,) + out.shape, jnp.float32),
            in_specs=[hbm] * 5,
            out_specs=vmem,
            scratch_shapes=[
                pltpu.SMEM((visits,), jnp.float32),
                pltpu.SMEM((visits, own), jnp.int32),
                pltpu.VMEM((visits, own * rows, columns), jnp.bfloat16),
                pltpu.VMEM((bands, visits, columns, width), jnp.bfloat16),
                pltpu.VMEM((entries, rows // 16, columns), jnp.int32),
                dma((bands + 4,)),
                pltpu.VMEM(blocks, jnp.bfloat16), pltpu.VMEM(flags, jnp.int32),
                pltpu.VMEM(blocks, jnp.bfloat16), pltpu.VMEM(flags, jnp.int32),
                pltpu.VMEM(blocks, jnp.bfloat16), pltpu.VMEM(flags, jnp.int32),
                pltpu.VMEM((1, long), jnp.int32),
                pltpu.VMEM((depth, 1, long), jnp.int32), pltpu.VMEM((depth, 1, long), jnp.int32),
                pltpu.VMEM((parts, 3, PATCH_DEV, slab, width), jnp.float32),
                pltpu.VMEM((parts, 3, PATCH_DEV, 5, slab, width), jnp.bfloat16),
                pltpu.VMEM((parts, 2, PATCH_DEV, slab, width), jnp.float32),
                pltpu.VMEM((parts, 2, PATCH_DEV, 5, slab, width), jnp.bfloat16),
                pltpu.SMEM((2, depth, 1, long), jnp.int32),
                pltpu.VMEM((PATCH_DEV, 6, slab, width), jnp.float32),
                pltpu.VMEM(work + blocks[3:], jnp.bfloat16), pltpu.VMEM(work + flags[3:], jnp.int32),
                dma((parts, depth)), dma((parts, depth)), dma((parts // 2, depth)), dma((parts // 2, depth)),
                dma((depth,)), dma((depth,)), dma((depth,)), dma((depth,)),
                dma((parts, depth)), dma((parts, depth)), dma((parts // 2, depth)), dma((parts // 2, depth)),
                dma((parts,)), dma((parts,)), dma((parts // 2,)), dma((parts // 2,)),
                dma((parts, 3)), dma((parts, 2)), dma((parts, 3)), dma((parts, 2)), dma((2,)),
            ],
            compiler_params=pltpu.CompilerParams(
                collective_id=0, has_side_effects=True, vmem_limit_bytes=24 * 1024 * 1024
            ),
        )(*[pltpu.with_memory_space_constraint(x, pltpu.HBM) for x in (
            flux_scale, patch_lists, visit_tiles.reshape(visits, own * rows, columns), warp_matrix,
            clip_bits.reshape(entries, rows // 16, columns))])
        return pl.pallas_call(
            split, out_shape=(out, out), in_specs=[vmem], out_specs=(hbm, hbm),
            scratch_shapes=[dma((2,))],
            compiler_params=pltpu.CompilerParams(vmem_limit_bytes=8 * 1024 * 1024),
        )(both)
    targets = patch_lists.reshape(entries)
    number = jnp.arange(entries, dtype=jnp.int32)
    same = (targets[:, None] == targets[None, :]) & (number[None, :] < number[:, None])
    rank = jnp.sum(same.astype(jnp.int32), axis=1)
    slot = targets * CAPACITY + rank
    source = jnp.min(
        jnp.where(slot[None, :] == jnp.arange(patches * CAPACITY, dtype=jnp.int32)[:, None], number[None, :], entries),
        axis=1,
    )
    return pl.pallas_call(
        functools.partial(kernel, sky, depth),
        out_shape=(out, out),
        in_specs=[smem, smem, vmem, vmem, vmem],
        out_specs=(vmem, vmem),
        scratch_shapes=[
            pltpu.VMEM((entries, rows, columns), jnp.bfloat16),
            pltpu.VMEM((devices, SLOTS, share, columns), jnp.bfloat16),
            pltpu.VMEM((devices, SLOTS, share // 16, columns), jnp.int32),
            pltpu.VMEM((devices, SLOTS, share, columns), jnp.bfloat16),
            pltpu.VMEM((devices, SLOTS, share // 16, columns), jnp.int32),
            pltpu.VMEM((PATCH_DEV, 6, share, columns), jnp.float32),
        ] + [pltpu.SemaphoreType.DMA((devices,))] * 4,
        compiler_params=pltpu.CompilerParams(
            collective_id=0, has_side_effects=True, vmem_limit_bytes=67043328 - 1048576
        ),
    )(flux_scale, source, visit_tiles.reshape(visits, own * rows, columns), warp_matrix,
      clip_bits.reshape(entries, rows // 16, columns))


def solution(mesh):
    whole = ("tracts", "sky", "depth")
    placed = (P(whole, None, None, None), P(whole, None, None), P(whole), P(whole, None), P(whole, None, None, None))
    outs = P(None, ("tracts", "sky"), "depth", None)
    return jax.shard_map(
        functools.partial(per_device, mesh.shape["sky"], mesh.shape["depth"]),
        mesh=mesh,
        in_specs=placed,
        out_specs=(outs, outs),
        check_vma=False,
    )
```

```python
import functools

import jax
import jax.numpy as jnp
from jax import lax
from jax.experimental import pallas as pl
from jax.experimental.pallas import tpu as pltpu
from jax.sharding import PartitionSpec as P

PATCH_DEV = 4
CAPACITY = 2
SLOTS = PATCH_DEV * CAPACITY
MESH = pl.DeviceIdType.MESH
STEP = 4
LAG = 3
LEAD = 2


def kernel(sky, depth, scale_ref, src_ref, tiles_ref, matrix_ref, bits_ref, mean_ref, var_ref,
           warped, send_t, send_b, recv_t, recv_b, acc, st, sb, rt, rb):
    z, d = lax.axis_index("sky"), lax.axis_index("depth")
    me = z * depth + d
    devices = sky * depth
    visits, entries_rows, columns = tiles_ref.shape
    entries, rows, _ = warped.shape
    share = rows // depth

    def place(j):
        return lax.div(lax.rem(me + j, devices), depth), lax.rem(lax.rem(me + j, devices), depth)

    barrier = pltpu.get_barrier_semaphore()

    def greet(j, _):
        zz, dd = place(j)
        pl.semaphore_signal(barrier, inc=1, device_id={"sky": zz, "depth": dd}, device_id_type=MESH)
        return 0

    lax.fori_loop(1, devices, greet, 0)

    per_visit = entries // visits
    for v in range(visits):
        def warp(i, _, v=v):
            start = pl.multiple_of(i * STEP * rows, STEP * rows)
            product = jnp.dot(tiles_ref[v, pl.ds(start, STEP * rows), :], matrix_ref[v],
                              preferred_element_type=jnp.float32) * scale_ref[v]
            warped[pl.ds(v * per_visit + i * STEP, STEP)] = product.astype(jnp.bfloat16).reshape(STEP, rows, columns)
            return 0
        lax.fori_loop(0, per_visit // STEP, warp, 0)

    pl.semaphore_wait(barrier, devices - 1)

    def copies(zz, dd, there, mine):
        to = {"sky": zz, "depth": dd}
        return (
            pltpu.make_async_remote_copy(src_ref=send_t.at[there], dst_ref=recv_t.at[mine], send_sem=st.at[there],
                                         recv_sem=rt.at[mine], device_id=to, device_id_type=MESH),
            pltpu.make_async_remote_copy(src_ref=send_b.at[there], dst_ref=recv_b.at[mine], send_sem=sb.at[there],
                                         recv_sem=rb.at[mine], device_id=to, device_id_type=MESH),
        )

    def post(jj, _):
        zz = lax.rem(z + sky // 2 + jj, sky)

        def fill(s, _):
            e = src_ref[zz * SLOTS + s]
            valid = (e < entries).astype(jnp.int32)
            e = jnp.minimum(e, entries - 1)
            block = warped[e]
            flags = bits_ref[e] * valid
            for dd in range(depth):
                send_t[zz * depth + dd, s] = block[dd * share:(dd + 1) * share]
                send_b[zz * depth + dd, s] = flags[dd * (share // 16):(dd + 1) * (share // 16)]
            return 0

        lax.fori_loop(0, SLOTS, fill, 0)

        def start(k, _):
            dd = lax.rem(d + k, depth)
            there = zz * depth + dd

            @pl.when(there != me)
            def _():
                for c in copies(zz, dd, there, me):
                    c.start()
            return 0

        lax.fori_loop(0, depth, start, 0)
        return 0

    lax.fori_loop(0, sky, post, 0)

    acc[...] = jnp.zeros_like(acc)
    position = lax.rem(lax.broadcasted_iota(jnp.int32, (share, columns), 0), 16)

    def add(tiles, flags, source):
        for p in range(PATCH_DEV):
            sums = [acc[p, q] for q in range(6)]
            for c in range(CAPACITY):
                w = tiles[source, p * CAPACITY + c].astype(jnp.float32)
                packed = flags[source, p * CAPACITY + c]
                packed = jnp.broadcast_to(packed[:, None, :], (share // 16, 16, columns)).reshape(share, columns)
                shifted = lax.shift_right_logical(packed, position)
                first = (shifted & 1).astype(jnp.float32)
                both = first * (lax.shift_right_logical(shifted, 16) & 1).astype(jnp.float32)
                fw, bw = first * w, both * w
                for q, term in enumerate((first, fw, fw * w, both, bw, bw * w)):
                    sums[q] = sums[q] + term
            for q in range(6):
                acc[p, q] = sums[q]

    add(send_t, send_b, me)

    def take(jj, _):
        zz = lax.rem(z - sky // 2 - jj + 2 * sky, sky)

        def one(k, _):
            dd = lax.rem(d - k + depth, depth)
            there = zz * depth + dd

            @pl.when(there != me)
            def _():
                for c in copies(zz, dd, there, there):
                    c.wait_recv()
                add(recv_t, recv_b, there)
            return 0

        lax.fori_loop(0, depth, one, 0)
        return 0

    lax.fori_loop(0, sky, take, 0)

    for p in range(PATCH_DEV):
        cf, sf, qf, cb, sb_, qb = [acc[p, q] for q in range(6)]
        mean = sf / jnp.maximum(cf, 1.0)
        shift = sb_ - mean * cb
        square = qb - mean * sb_ - mean * shift
        step = shift / jnp.maximum(cb, 1.0)
        mean_ref[0, p] = mean
        mean_ref[1, p] = mean + step
        var_ref[0, p] = (qf - sf * mean) / jnp.maximum(cf - 1.0, 1.0)
        var_ref[1, p] = (square - shift * step) / jnp.maximum(cb - 1.0, 1.0)

    def drain(j, _):
        zz, dd = place(j)
        for c in copies(zz, dd, zz * depth + dd, me):
            c.wait_send()
        return 0

    lax.fori_loop(1, devices, drain, 0)


def folded(depth, scale_hbm, lists_hbm, tiles_hbm, matrix_hbm, bits_hbm, out_ref,
           scale_ref, lists_ref, tiles_ref, matrix_ref, bits_ref, s_in,
           out_t, out_b, row_t, row_b, raw_t, raw_b, own_s, held_s, far32, far16, got32, got16, tables, local,
           work_t, work_b, s_x, s_y, s_s, r_x, r_y, r_s, r_g, s_l):
    z, d = lax.axis_index("sky"), lax.axis_index("depth")
    half = z // 2
    rem = z - 2 * half
    inner, outer = rem != half, rem == half
    mate = 2 * half + 1 - rem
    across, beyond = 3 - z, 3 - mate
    base = d // 2 * 2
    other = depth - 2 - base
    parts, _, entries, slab, width = out_t.shape
    groups_here = out_b.shape[0] * width // tiles_ref.shape[2]
    visits, entries_rows, columns = tiles_ref.shape
    per_visit = entries // visits
    rows = entries_rows // per_visit
    share = rows // depth
    slabs = share // slab
    long = own_s.shape[1]

    bands = matrix_ref.shape[0]
    tiles_in = pltpu.make_async_copy(tiles_hbm, tiles_ref, s_in.at[bands])
    bits_in = pltpu.make_async_copy(bits_hbm, bits_ref, s_in.at[bands + 1])
    scale_in = pltpu.make_async_copy(scale_hbm, scale_ref, s_in.at[bands + 2])
    lists_in = pltpu.make_async_copy(lists_hbm, lists_ref, s_in.at[bands + 3])

    def matrix_in(band):
        lanes = pl.ds(band * width, width)
        return pltpu.make_async_copy(matrix_hbm.at[:, :, lanes], matrix_ref.at[band], s_in.at[band])

    barrier = pltpu.get_barrier_semaphore()
    for k in range(1, depth):
        pl.semaphore_signal(barrier, inc=1, device_id={"depth": lax.rem(d + k, depth)}, device_id_type=MESH)
    for k in range(depth):
        pl.semaphore_signal(barrier, inc=1, device_id={"sky": mate, "depth": k}, device_id_type=MESH)
    pl.semaphore_signal(barrier, inc=1, device_id={"sky": beyond}, device_id_type=MESH)

    @pl.when(inner)
    def _():
        pl.semaphore_signal(barrier, inc=1, device_id={"sky": across}, device_id_type=MESH)

    tiles_in.start()
    matrix_in(0).start()
    lists_in.start()
    scale_in.start()
    bits_in.start()
    for band in range(1, bands):
        matrix_in(band).start()

    def remote(src, dst, send, recv, to):
        return pltpu.make_async_remote_copy(src_ref=src, dst_ref=dst, send_sem=send, recv_sem=recv, device_id=to,
                                            device_id_type=MESH)

    def to_row(c, there):
        return remote(out_t.at[c, there], row_t.at[c, d], s_x.at[0], r_x.at[c], {"depth": there})

    def flags_to_row(b, there):
        return remote(out_b.at[b, there], row_b.at[b, d], s_x.at[1], r_x.at[2 * b], {"depth": there})

    def table_to_row(there):
        return remote(own_s, held_s.at[d], s_s.at[0], r_s.at[0], {"depth": there})

    def table_to_mates(there):
        return remote(own_s, held_s.at[depth + d], s_s.at[0], r_s.at[1], {"sky": mate, "depth": there})

    def direct(c, there):
        to = {"sky": mate, "depth": there}
        return remote(out_t.at[c, there], raw_t.at[c, d], s_y.at[0], r_y.at[c], to)

    def flags_direct(b, there):
        to = {"sky": mate, "depth": there}
        return remote(out_b.at[b, there], raw_b.at[b, d], s_y.at[1], r_y.at[2 * b], to)

    def onward(c):
        pair = pl.ds(other, 2)
        return remote(row_t.at[c, pair], raw_t.at[c, pair], s_y.at[0], r_y.at[c], {"sky": mate})

    def flags_onward(b):
        pair = pl.ds(other, 2)
        return remote(row_b.at[b, pair], raw_b.at[b, pair], s_y.at[1], r_y.at[2 * b], {"sky": mate})

    def sums_to(c, t, where, slot):
        to = {"sky": where}
        return (remote(far32.at[c, t], got32.at[c, slot], s_y.at[0], r_g.at[c], to),
                remote(far16.at[c, t], got16.at[c, slot], s_y.at[1], r_g.at[c], to))

    def arrived(ref, sem):
        remote(ref, ref, s_x.at[0], sem, {"sky": mate}).wait_recv()

    def left(ref, sem):
        remote(ref, ref, sem, r_s.at[0], {"sky": mate}).wait_send()

    def row_arrived(c):
        @pl.when(c % 2 == 0)
        def _():
            arrived(out_t.at[0, :, pl.ds(0, entries * 15 // 16)], r_x.at[c])

        @pl.when(c % 2 == 1)
        def _():
            arrived(out_t.at[0, pl.ds(0, depth - 1)], r_x.at[c])

    def raw_arrived(c):
        @pl.when(c % 2 == 0)
        def _():
            arrived(out_t.at[pl.ds(0, depth + 1), 0], r_y.at[c])

        @pl.when(c % 2 == 1)
        def _():
            arrived(out_t.at[0], r_y.at[c])

    def sums_arrived(c, slots):
        arrived(out_t.at[0, pl.ds(0, 2 * slots), pl.ds(0, PATCH_DEV * 7 // 2)], r_g.at[c])

    position = lax.broadcasted_iota(jnp.int32, (slab, width), 0)
    for which in range(2):
        for dd in range(depth):
            work_t[which, dd, entries] = jnp.zeros((slab, width), jnp.bfloat16)
            work_b[which, dd, entries] = jnp.zeros((1, width), jnp.int32)

    lists_in.wait()
    lane = lax.broadcasted_iota(jnp.int32, (1, long), 1)
    table = jnp.full((1, long), entries, jnp.int32)
    targets = [lists_ref[v, k] for v in range(visits) for k in range(per_visit)]
    for e in range(entries):
        rank = jnp.int32(0)
        for f in range(e // per_visit * per_visit):
            rank = rank + (targets[e] == targets[f]).astype(jnp.int32)
        table = jnp.where(lane == targets[e] * CAPACITY + rank, e, table)
    own_s[...] = table
    held_s[d] = table

    def stage(c, which, tiles, flags):
        work_t[which, :, :entries] = tiles[c]
        work_b[which, :, :entries] = flags[c // 2]

    def gather(c, patch, groups):
        place = position + (c % 2) * slab
        sums = [jnp.zeros((slab, width), jnp.float32)] * 6
        for which in range(groups):
            for dd in range(depth):
                for k in range(CAPACITY):
                    e = tables[which, dd, 0, patch * CAPACITY + k]
                    w = work_t[which, dd, e].astype(jnp.float32)
                    packed = jnp.broadcast_to(work_b[which, dd, e], (slab, width))
                    shifted = lax.shift_right_logical(packed, place)
                    first = (shifted & 1).astype(jnp.float32)
                    both = first * (lax.shift_right_logical(shifted, 16) & 1).astype(jnp.float32)
                    fw, bw = first * w, both * w
                    sums = [a + b for a, b in zip(sums, (first, fw, fw * w, both, bw, bw * w))]
        return sums

    def send_sums(c, t, where, groups):
        def one(p, _):
            cf, sf, qf, cb, sb, qb = gather(c, where * PATCH_DEV + p, groups)
            mean = sf / jnp.maximum(cf, 1.0)
            far32[c, t, p] = sf
            packed = (cf, cb, qf - sf * mean, sb - mean * cb, qb - sb * (sb / jnp.maximum(cb, 1.0)))
            for q, value in enumerate(packed):
                far16[c, t, p, q] = value.astype(jnp.bfloat16)
            return 0
        lax.fori_loop(0, PATCH_DEV, one, 0)
        for copy in sums_to(c, t, where, half):
            copy.start()

    def send_direct(c):
        @pl.when(c % 2 == 0)
        def _():
            for j in range(2):
                flags_direct(c // 2, base + j).start()
        for j in range(2):
            direct(c, base + j).start()

    def warp(column, _):
        lanes = pl.ds(pl.multiple_of(column * width, width), width)
        for band in range(bands):
            @pl.when(column == band)
            def _(band=band):
                matrix_in(band).wait()
        for v in range(visits):
            product = jnp.dot(tiles_ref[v], matrix_ref[column, v], preferred_element_type=jnp.float32)
            block = (product * scale_ref[v]).reshape(per_visit, depth, slabs, slab, width)
            for dd in range(depth):
                for h in range(slabs):
                    out_t[column * slabs + h, dd, v * per_visit:(v + 1) * per_visit] = block[:, dd, h].astype(jnp.bfloat16)
        for g in range(groups_here):
            b = column * groups_here + g
            for dd in range(depth):
                line = dd * groups_here + g
                out_b[b, dd] = bits_ref[:, line:line + 1, lanes]
            row_b[b, d] = out_b[b, d]
        for h in range(slabs):
            row_t[column * slabs + h, d] = out_t[column * slabs + h, d]

        @pl.when(column == 0)
        def _():
            @pl.when(inner)
            def _():
                pl.semaphore_wait(barrier, 2 * depth + 1)

            @pl.when(outer)
            def _():
                pl.semaphore_wait(barrier, 2 * depth)
            for k in range(1, depth):
                table_to_row(lax.rem(d + k, depth)).start()

            @pl.when(outer)
            def _():
                for k in range(depth):
                    table_to_mates(k).start()

        for h in range(slabs):
            for k in range(1, depth):
                there = lax.rem(d + k, depth)
                if h % 2 == 0:
                    flags_to_row(column * groups_here + h // 2, there).start()
                to_row(column * slabs + h, there).start()

            @pl.when(jnp.logical_and(outer, column * slabs + h < LEAD))
            def _(h=h):
                send_direct(column * slabs + h)
        return 0

    tiles_in.wait()
    scale_in.wait()
    bits_in.wait()
    lax.fori_loop(0, bands, warp, 0)
    mine, theirs = (row_t, row_b), (raw_t, raw_b)

    arrived(held_s.at[pl.ds(0, depth - 1)], r_s.at[0])
    held = pltpu.make_async_copy(held_s.at[pl.ds(0, depth)], tables.at[0], s_l.at[0])
    held.start()
    held.wait()

    def total(c, slot, p):
        sf = got32[c, slot, p]
        cf, cb, mf, shift, mb = [got16[c, slot, p, q].astype(jnp.float32) for q in range(5)]
        mean = sf / jnp.maximum(cf, 1.0)
        sb = shift + mean * cb
        return cf, sf, mf + sf * mean, cb, sb, mb + sb * (sb / jnp.maximum(cb, 1.0))

    def finish(c):
        lanes = pl.ds(pl.multiple_of(c // slabs * width, width), width)
        lines = pl.ds(pl.multiple_of(c % slabs * slab, slab), slab)
        stage(c, 0, *mine)

        @pl.when(inner)
        def _():
            stage(c, 1, *theirs)

            def one(p, _):
                for q, value in enumerate(gather(c, z * PATCH_DEV + p, 2)):
                    local[p, q] = value
                return 0
            lax.fori_loop(0, PATCH_DEV, one, 0)
            sums_arrived(c, 1)

        @pl.when(outer)
        def _():
            def one(p, _):
                for q, value in enumerate(gather(c, z * PATCH_DEV + p, 1)):
                    local[p, q] = value
                return 0
            lax.fori_loop(0, PATCH_DEV, one, 0)
            sums_arrived(c, 2)
            for p in range(PATCH_DEV):
                for q, value in enumerate(total(c, half, p)):
                    local[p, q] = local[p, q] + value

        for p in range(PATCH_DEV):
            cf, sf, qf, cb, sb, qb = [local[p, q] + value for q, value in enumerate(total(c, 1 - half, p))]
            mean = sf / jnp.maximum(cf, 1.0)
            shift = sb - mean * cb
            square = qb - mean * sb - mean * shift
            step = shift / jnp.maximum(cb, 1.0)
            out_ref[0, 0, p, lines, lanes] = mean
            out_ref[0, 1, p, lines, lanes] = mean + step
            out_ref[1, 0, p, lines, lanes] = (qf - sf * mean) / jnp.maximum(cf - 1.0, 1.0)
            out_ref[1, 1, p, lines, lanes] = (square - shift * step) / jnp.maximum(cb - 1.0, 1.0)

    def forward(c, _):
        row_arrived(c)

        @pl.when(outer)
        def _():
            @pl.when(c % 2 == 0)
            def _():
                flags_onward(c // 2).start()
            onward(c).start()

            @pl.when(jnp.logical_and(c >= 1, c + 1 < parts))
            def _():
                send_direct(c + 1)

        @pl.when(inner)
        def _():
            stage(c, 0, *mine)
            send_sums(c, 2, mate, 1)

            @pl.when(c == 0)
            def _():
                arrived(held_s.at[pl.ds(0, depth)], r_s.at[1])
                more = pltpu.make_async_copy(held_s.at[pl.ds(depth, depth)], tables.at[1], s_l.at[1])
                more.start()
                more.wait()

            raw_arrived(c)
            stage(c, 1, *theirs)
            send_sums(c, 0, beyond, 2)
            send_sums(c, 1, across, 2)

            @pl.when(c >= LAG)
            def _():
                finish(c - LAG)
        return 0

    lax.fori_loop(0, parts, forward, 0)

    def close(c, _):
        @pl.when(jnp.logical_or(outer, c >= parts - LAG))
        def _():
            finish(c)
        return 0

    lax.fori_loop(0, parts, close, 0)

    left(out_t.at[:, pl.ds(0, depth - 1)], s_x.at[0])
    left(out_b.at[:, pl.ds(0, depth - 1)], s_x.at[1])

    @pl.when(outer)
    def _():
        left(held_s.at[pl.ds(0, 2 * depth - 1)], s_s.at[0])
        left(out_t, s_y.at[0])
        left(out_b, s_y.at[1])

    @pl.when(inner)
    def _():
        left(held_s.at[pl.ds(0, depth - 1)], s_s.at[0])
        left(far32, s_y.at[0])
        left(far16, s_y.at[1])


def split(both_ref, mean_hbm, var_hbm, sems):
    copies = [pltpu.make_async_copy(both_ref.at[q], out, sems.at[q]) for q, out in enumerate((mean_hbm, var_hbm))]
    for copy in copies:
        copy.start()
    for copy in copies:
        copy.wait()


def per_device(sky, depth, visit_tiles, warp_matrix, flux_scale, patch_lists, clip_bits):
    visits, own, rows, columns = visit_tiles.shape
    entries = visits * own
    patches = PATCH_DEV * sky
    devices = sky * depth
    share = rows // depth
    smem, vmem = pl.BlockSpec(memory_space=pltpu.SMEM), pl.BlockSpec(memory_space=pltpu.VMEM)
    hbm = pl.BlockSpec(memory_space=pltpu.HBM)
    out = jax.ShapeDtypeStruct((2, PATCH_DEV, share, columns), jnp.float32)
    if sky == 4 and depth == 4:
        width = 128
        slab = 8
        bands = columns // width
        parts = bands * (share // slab)
        long = -(-patches * CAPACITY // 128) * 128
        blocks = (parts, depth, entries, slab, width)
        flags = (parts // 2, depth, entries, 1, width)
        work = (2, depth, entries + 1)
        dma = pltpu.SemaphoreType.DMA
        both = pl.pallas_call(
            functools.partial(folded, depth),
            out_shape=jax.ShapeDtypeStruct((2,) + out.shape, jnp.float32),
            in_specs=[hbm] * 5,
            out_specs=vmem,
            scratch_shapes=[
                pltpu.SMEM((visits,), jnp.float32),
                pltpu.SMEM((visits, own), jnp.int32),
                pltpu.VMEM((visits, own * rows, columns), jnp.bfloat16),
                pltpu.VMEM((bands, visits, columns, width), jnp.bfloat16),
                pltpu.VMEM((entries, rows // 16, columns), jnp.int32),
                dma((bands + 4,)),
                pltpu.VMEM(blocks, jnp.bfloat16), pltpu.VMEM(flags, jnp.int32),
                pltpu.VMEM(blocks, jnp.bfloat16), pltpu.VMEM(flags, jnp.int32),
                pltpu.VMEM(blocks, jnp.bfloat16), pltpu.VMEM(flags, jnp.int32),
                pltpu.VMEM((1, long), jnp.int32), pltpu.VMEM((2 * depth, 1, long), jnp.int32),
                pltpu.VMEM((parts, 3, PATCH_DEV, slab, width), jnp.float32),
                pltpu.VMEM((parts, 3, PATCH_DEV, 5, slab, width), jnp.bfloat16),
                pltpu.VMEM((parts, 2, PATCH_DEV, slab, width), jnp.float32),
                pltpu.VMEM((parts, 2, PATCH_DEV, 5, slab, width), jnp.bfloat16),
                pltpu.SMEM((2, depth, 1, long), jnp.int32),
                pltpu.VMEM((PATCH_DEV, 6, slab, width), jnp.float32),
                pltpu.VMEM(work + blocks[3:], jnp.bfloat16), pltpu.VMEM(work + flags[3:], jnp.int32),
                dma((2,)), dma((2,)), dma((1,)), dma((parts,)), dma((parts,)), dma((2,)), dma((parts,)), dma((2,)),
            ],
            compiler_params=pltpu.CompilerParams(
                collective_id=0, has_side_effects=True, vmem_limit_bytes=24 * 1024 * 1024
            ),
        )(*[pltpu.with_memory_space_constraint(x, pltpu.HBM) for x in (
            flux_scale, patch_lists, visit_tiles.reshape(visits, own * rows, columns), warp_matrix,
            clip_bits.reshape(entries, rows // 16, columns))])
        return pl.pallas_call(
            split, out_shape=(out, out), in_specs=[vmem], out_specs=(hbm, hbm),
            scratch_shapes=[dma((2,))],
            compiler_params=pltpu.CompilerParams(vmem_limit_bytes=8 * 1024 * 1024),
        )(both)
    targets = patch_lists.reshape(entries)
    number = jnp.arange(entries, dtype=jnp.int32)
    same = (targets[:, None] == targets[None, :]) & (number[None, :] < number[:, None])
    rank = jnp.sum(same.astype(jnp.int32), axis=1)
    slot = targets * CAPACITY + rank
    source = jnp.min(
        jnp.where(slot[None, :] == jnp.arange(patches * CAPACITY, dtype=jnp.int32)[:, None], number[None, :], entries),
        axis=1,
    )
    return pl.pallas_call(
        functools.partial(kernel, sky, depth),
        out_shape=(out, out),
        in_specs=[smem, smem, vmem, vmem, vmem],
        out_specs=(vmem, vmem),
        scratch_shapes=[
            pltpu.VMEM((entries, rows, columns), jnp.bfloat16),
            pltpu.VMEM((devices, SLOTS, share, columns), jnp.bfloat16),
            pltpu.VMEM((devices, SLOTS, share // 16, columns), jnp.int32),
            pltpu.VMEM((devices, SLOTS, share, columns), jnp.bfloat16),
            pltpu.VMEM((devices, SLOTS, share // 16, columns), jnp.int32),
            pltpu.VMEM((PATCH_DEV, 6, share, columns), jnp.float32),
        ] + [pltpu.SemaphoreType.DMA((devices,))] * 4,
        compiler_params=pltpu.CompilerParams(
            collective_id=0, has_side_effects=True, vmem_limit_bytes=67043328 - 1048576
        ),
    )(flux_scale, source, visit_tiles.reshape(visits, own * rows, columns), warp_matrix,
      clip_bits.reshape(entries, rows // 16, columns))


def solution(mesh):
    whole = ("tracts", "sky", "depth")
    placed = (P(whole, None, None, None), P(whole, None, None), P(whole), P(whole, None), P(whole, None, None, None))
    outs = P(None, ("tracts", "sky"), "depth", None)
    return jax.shard_map(
        functools.partial(per_device, mesh.shape["sky"], mesh.shape["depth"]),
        mesh=mesh,
        in_specs=placed,
        out_specs=(outs, outs),
        check_vma=False,
    )
```

```python
import functools

import jax
import jax.numpy as jnp
from jax import lax
from jax.experimental import pallas as pl
from jax.experimental.pallas import tpu as pltpu
from jax.sharding import PartitionSpec as P

PATCH_DEV = 4
CAPACITY = 2
SLOTS = PATCH_DEV * CAPACITY
MESH = pl.DeviceIdType.MESH
STEP = 4
LAG = 5
LEAD = 5
SLAB = 4
SWAP = 2
TURN = 5


def kernel(sky, depth, scale_ref, src_ref, tiles_ref, matrix_ref, bits_ref, mean_ref, var_ref,
           warped, send_t, send_b, recv_t, recv_b, acc, st, sb, rt, rb):
    z, d = lax.axis_index("sky"), lax.axis_index("depth")
    me = z * depth + d
    devices = sky * depth
    visits, entries_rows, columns = tiles_ref.shape
    entries, rows, _ = warped.shape
    share = rows // depth

    def place(j):
        return lax.div(lax.rem(me + j, devices), depth), lax.rem(lax.rem(me + j, devices), depth)

    barrier = pltpu.get_barrier_semaphore()

    def greet(j, _):
        zz, dd = place(j)
        pl.semaphore_signal(barrier, inc=1, device_id={"sky": zz, "depth": dd}, device_id_type=MESH)
        return 0

    lax.fori_loop(1, devices, greet, 0)

    per_visit = entries // visits
    for v in range(visits):
        def warp(i, _, v=v):
            start = pl.multiple_of(i * STEP * rows, STEP * rows)
            product = jnp.dot(tiles_ref[v, pl.ds(start, STEP * rows), :], matrix_ref[v],
                              preferred_element_type=jnp.float32) * scale_ref[v]
            warped[pl.ds(v * per_visit + i * STEP, STEP)] = product.astype(jnp.bfloat16).reshape(STEP, rows, columns)
            return 0
        lax.fori_loop(0, per_visit // STEP, warp, 0)

    pl.semaphore_wait(barrier, devices - 1)

    def copies(zz, dd, there, mine):
        to = {"sky": zz, "depth": dd}
        return (
            pltpu.make_async_remote_copy(src_ref=send_t.at[there], dst_ref=recv_t.at[mine], send_sem=st.at[there],
                                         recv_sem=rt.at[mine], device_id=to, device_id_type=MESH),
            pltpu.make_async_remote_copy(src_ref=send_b.at[there], dst_ref=recv_b.at[mine], send_sem=sb.at[there],
                                         recv_sem=rb.at[mine], device_id=to, device_id_type=MESH),
        )

    def post(jj, _):
        zz = lax.rem(z + sky // 2 + jj, sky)

        def fill(s, _):
            e = src_ref[zz * SLOTS + s]
            valid = (e < entries).astype(jnp.int32)
            e = jnp.minimum(e, entries - 1)
            block = warped[e]
            flags = bits_ref[e] * valid
            for dd in range(depth):
                send_t[zz * depth + dd, s] = block[dd * share:(dd + 1) * share]
                send_b[zz * depth + dd, s] = flags[dd * (share // 16):(dd + 1) * (share // 16)]
            return 0

        lax.fori_loop(0, SLOTS, fill, 0)

        def start(k, _):
            dd = lax.rem(d + k, depth)
            there = zz * depth + dd

            @pl.when(there != me)
            def _():
                for c in copies(zz, dd, there, me):
                    c.start()
            return 0

        lax.fori_loop(0, depth, start, 0)
        return 0

    lax.fori_loop(0, sky, post, 0)

    acc[...] = jnp.zeros_like(acc)
    position = lax.rem(lax.broadcasted_iota(jnp.int32, (share, columns), 0), 16)

    def add(tiles, flags, source):
        for p in range(PATCH_DEV):
            sums = [acc[p, q] for q in range(6)]
            for c in range(CAPACITY):
                w = tiles[source, p * CAPACITY + c].astype(jnp.float32)
                packed = flags[source, p * CAPACITY + c]
                packed = jnp.broadcast_to(packed[:, None, :], (share // 16, 16, columns)).reshape(share, columns)
                shifted = lax.shift_right_logical(packed, position)
                first = (shifted & 1).astype(jnp.float32)
                both = first * (lax.shift_right_logical(shifted, 16) & 1).astype(jnp.float32)
                fw, bw = first * w, both * w
                for q, term in enumerate((first, fw, fw * w, both, bw, bw * w)):
                    sums[q] = sums[q] + term
            for q in range(6):
                acc[p, q] = sums[q]

    add(send_t, send_b, me)

    def take(jj, _):
        zz = lax.rem(z - sky // 2 - jj + 2 * sky, sky)

        def one(k, _):
            dd = lax.rem(d - k + depth, depth)
            there = zz * depth + dd

            @pl.when(there != me)
            def _():
                for c in copies(zz, dd, there, there):
                    c.wait_recv()
                add(recv_t, recv_b, there)
            return 0

        lax.fori_loop(0, depth, one, 0)
        return 0

    lax.fori_loop(0, sky, take, 0)

    for p in range(PATCH_DEV):
        cf, sf, qf, cb, sb_, qb = [acc[p, q] for q in range(6)]
        mean = sf / jnp.maximum(cf, 1.0)
        shift = sb_ - mean * cb
        square = qb - mean * sb_ - mean * shift
        step = shift / jnp.maximum(cb, 1.0)
        mean_ref[0, p] = mean
        mean_ref[1, p] = mean + step
        var_ref[0, p] = (qf - sf * mean) / jnp.maximum(cf - 1.0, 1.0)
        var_ref[1, p] = (square - shift * step) / jnp.maximum(cb - 1.0, 1.0)

    def drain(j, _):
        zz, dd = place(j)
        for c in copies(zz, dd, zz * depth + dd, me):
            c.wait_send()
        return 0

    lax.fori_loop(1, devices, drain, 0)


def folded(depth, scale_hbm, lists_hbm, tiles_hbm, matrix_hbm, bits_hbm, out_ref,
           scale_ref, lists_ref, tiles_ref, matrix_ref, bits_ref, s_in,
           out_t, out_b, row_t, row_b, raw_t, raw_b, own_s, held_s, far32, far16, got32, got16, tables, local,
           work_t, work_b, s_x, s_y, s_s, r_x, r_y, r_s, r_g, s_l):
    z, d = lax.axis_index("sky"), lax.axis_index("depth")
    half = z // 2
    rem = z - 2 * half
    inner, outer = rem != half, rem == half
    mate = 2 * half + 1 - rem
    across, beyond = 3 - z, 3 - mate
    base = d // 2 * 2
    other = depth - 2 - base
    twin = 2 * base + 1 - d
    parts, _, entries, slab, width = out_t.shape
    visits, entries_rows, columns = tiles_ref.shape
    per_visit = entries // visits
    rows = entries_rows // per_visit
    share = rows // depth
    slabs = share // slab
    long = own_s.shape[1]

    bands = matrix_ref.shape[0]
    first = bands // 2 * slabs - SWAP
    chain = parts - SWAP

    def chunk(i):
        return i + jnp.where(i >= first, SWAP, 0)

    def swapped(c):
        return jnp.logical_and(c >= first, c < first + SWAP)

    def fresh(c):
        return jnp.logical_or(c % slabs == 0, c == first)

    tiles_in = pltpu.make_async_copy(tiles_hbm, tiles_ref, s_in.at[bands])
    bits_in = pltpu.make_async_copy(bits_hbm, bits_ref, s_in.at[bands + 1])
    scale_in = pltpu.make_async_copy(scale_hbm, scale_ref, s_in.at[bands + 2])
    lists_in = pltpu.make_async_copy(lists_hbm, lists_ref, s_in.at[bands + 3])

    def matrix_in(band):
        lanes = pl.ds(band * width, width)
        return pltpu.make_async_copy(matrix_hbm.at[:, :, lanes], matrix_ref.at[band], s_in.at[band])

    barrier = pltpu.get_barrier_semaphore()
    for k in range(1, depth):
        pl.semaphore_signal(barrier, inc=1, device_id={"depth": lax.rem(d + k, depth)}, device_id_type=MESH)
    for k in range(depth):
        pl.semaphore_signal(barrier, inc=1, device_id={"sky": mate, "depth": k}, device_id_type=MESH)
    for far in (across, beyond):
        pl.semaphore_signal(barrier, inc=1, device_id={"sky": far}, device_id_type=MESH)

    tiles_in.start()
    matrix_in(0).start()
    lists_in.start()
    scale_in.start()
    bits_in.start()
    for band in range(1, bands):
        matrix_in(band).start()

    def remote(src, dst, send, recv, to):
        return pltpu.make_async_remote_copy(src_ref=src, dst_ref=dst, send_sem=send, recv_sem=recv, device_id=to,
                                            device_id_type=MESH)

    def to_row(c, there):
        return remote(out_t.at[c, there], row_t.at[c, d], s_x.at[0], r_x.at[c], {"depth": there})

    def flags_to_row(b, there):
        return remote(out_b.at[b, there], row_b.at[b, d], s_x.at[1], r_x.at[slabs * b], {"depth": there})

    def table_to_row(there):
        return remote(own_s, held_s.at[d], s_s.at[0], r_s.at[0], {"depth": there})

    def table_to_mates(there):
        return remote(own_s, held_s.at[depth + d], s_s.at[0], r_s.at[1], {"sky": mate, "depth": there})

    def direct(c, there):
        to = {"sky": mate, "depth": there}
        return remote(out_t.at[c, there], raw_t.at[c, d], s_y.at[0], r_y.at[c], to)

    def flags_direct(c, there):
        to = {"sky": mate, "depth": there}
        b = c // slabs
        return remote(out_b.at[b, there], raw_b.at[b, d], s_y.at[1], r_y.at[c], to)

    def onward(c):
        pair = pl.ds(other, 2)
        return remote(row_t.at[c, pair], raw_t.at[c, pair], s_y.at[0], r_y.at[c], {"sky": mate})

    def flags_onward(c):
        b, pair = c // slabs, pl.ds(other, 2)
        return remote(row_b.at[b, pair], raw_b.at[b, pair], s_y.at[1], r_y.at[c], {"sky": mate})

    def sums_to(c, t, where, slot):
        to = {"sky": where}
        return (remote(far32.at[c, t], got32.at[c, slot], s_y.at[2], r_g.at[c], to),
                remote(far16.at[c, t], got16.at[c, slot], s_y.at[3], r_g.at[c], to))

    def arrived(ref, sem):
        remote(ref, ref, s_x.at[0], sem, {"sky": mate}).wait_recv()

    def left(ref, sem):
        remote(ref, ref, sem, r_s.at[0], {"sky": mate}).wait_send()

    def volume(tiles):
        a, b, k = next((a, b, k) for a in range(1, parts + 1) for b in range(1, depth + 1)
                       for k in range(1, entries + 1) if a * b * k == tiles)
        return out_t.at[pl.ds(0, a), pl.ds(0, b), pl.ds(0, k)]

    def blocks_arrived(c, flags, sem, count):
        flag_tiles = 2 * entries // slab

        @pl.when(flags)
        def _():
            arrived(volume(count * (entries + flag_tiles)), sem.at[c])

        @pl.when(jnp.logical_not(flags))
        def _():
            arrived(volume(count * entries), sem.at[c])

    def row_arrived(c):
        blocks_arrived(c, c % slabs == 0, r_x, depth - 1)

    def raw_arrived(c):
        blocks_arrived(c, fresh(c), r_y, depth)

    def sums_arrived(c, slots):
        arrived(volume(slots * PATCH_DEV * 7), r_g.at[c])

    position = lax.broadcasted_iota(jnp.int32, (slab, width), 0)
    for which in range(2):
        for dd in range(depth):
            work_t[which, dd, entries] = jnp.zeros((slab, width), jnp.bfloat16)
            work_b[which, dd, entries] = jnp.zeros((1, width), jnp.int32)

    lists_in.wait()
    lane = lax.broadcasted_iota(jnp.int32, (1, long), 1)
    table = jnp.full((1, long), entries, jnp.int32)
    targets = [lists_ref[v, k] for v in range(visits) for k in range(per_visit)]
    for e in range(entries):
        rank = jnp.int32(0)
        for f in range(e // per_visit * per_visit):
            rank = rank + (targets[e] == targets[f]).astype(jnp.int32)
        table = jnp.where(lane == targets[e] * CAPACITY + rank, e, table)
    own_s[...] = table
    held_s[d] = table

    def stage(c, which, tiles, flags):
        work_t[which, :, :entries] = tiles[c]
        work_b[which, :, :entries] = flags[c // slabs]

    def gather(c, patch, groups):
        place = position + (c % slabs) * slab
        sums = [jnp.zeros((slab, width), jnp.float32)] * 6
        for which in range(groups):
            for dd in range(depth):
                for k in range(CAPACITY):
                    e = tables[which, dd, 0, patch * CAPACITY + k]
                    w = work_t[which, dd, e].astype(jnp.float32)
                    packed = jnp.broadcast_to(work_b[which, dd, e], (slab, width))
                    shifted = lax.shift_right_logical(packed, place)
                    first = (shifted & 1).astype(jnp.float32)
                    both = first * (lax.shift_right_logical(shifted, 16) & 1).astype(jnp.float32)
                    fw, bw = first * w, both * w
                    sums = [a + b for a, b in zip(sums, (first, fw, fw * w, both, bw, bw * w))]
        return sums

    def send_sums(c, t, where, groups):
        def one(p, _):
            cf, sf, qf, cb, sb, qb = gather(c, where * PATCH_DEV + p, groups)
            mean = sf / jnp.maximum(cf, 1.0)
            far32[c, t, p] = sf
            packed = (cf, cb, qf - sf * mean, sb - mean * cb, qb - sb * (sb / jnp.maximum(cb, 1.0)))
            for q, value in enumerate(packed):
                far16[c, t, p, q] = value.astype(jnp.bfloat16)
            return 0
        lax.fori_loop(0, PATCH_DEV, one, 0)
        for copy in sums_to(c, t, where, half):
            copy.start()

    def send_direct(c):
        @pl.when(fresh(c))
        def _():
            for j in range(2):
                flags_direct(c, base + j).start()
        for j in range(2):
            direct(c, base + j).start()

    def send_onward(c):
        @pl.when(fresh(c))
        def _():
            flags_onward(c).start()
        onward(c).start()

    def warp(column, _):
        lanes = pl.ds(pl.multiple_of(column * width, width), width)
        for band in range(bands):
            @pl.when(column == band)
            def _(band=band):
                matrix_in(band).wait()
        for v in range(visits):
            product = jnp.dot(tiles_ref[v], matrix_ref[column, v], preferred_element_type=jnp.float32)
            block = (product * scale_ref[v]).reshape(per_visit, depth, slabs, slab, width)
            for dd in range(depth):
                for h in range(slabs):
                    out_t[column * slabs + h, dd, v * per_visit:(v + 1) * per_visit] = block[:, dd, h].astype(jnp.bfloat16)
        for dd in range(depth):
            out_b[column, dd] = bits_ref[:, dd:dd + 1, lanes]
        row_b[column, d] = out_b[column, d]
        for h in range(slabs):
            row_t[column * slabs + h, d] = out_t[column * slabs + h, d]

        @pl.when(column == 0)
        def _():
            pl.semaphore_wait(barrier, 2 * depth + 1)

        for h in range(slabs):
            for there in (other, other + 1, twin):
                if h == 0:
                    flags_to_row(column, there).start()
                to_row(column * slabs + h, there).start()

            c = column * slabs + h

            @pl.when(jnp.logical_or(jnp.logical_and(outer, c < LEAD), jnp.logical_and(inner, swapped(c))))
            def _(c=c):
                send_direct(c)

            if h == 0:
                @pl.when(column == 0)
                def _():
                    for k in range(1, depth):
                        table_to_row(lax.rem(d + k, depth)).start()
                    for k in range(depth):
                        table_to_mates(k).start()
        return 0

    tiles_in.wait()
    scale_in.wait()
    bits_in.wait()
    lax.fori_loop(0, bands, warp, 0)
    mine, theirs = (row_t, row_b), (raw_t, raw_b)

    def row_tables():
        arrived(held_s.at[pl.ds(0, depth - 1)], r_s.at[0])
        held = pltpu.make_async_copy(held_s.at[pl.ds(0, depth)], tables.at[0], s_l.at[0])
        held.start()
        held.wait()

    def total(c, slot, p):
        sf = got32[c, slot, p]
        cf, cb, mf, shift, mb = [got16[c, slot, p, q].astype(jnp.float32) for q in range(5)]
        mean = sf / jnp.maximum(cf, 1.0)
        sb = shift + mean * cb
        return cf, sf, mf + sf * mean, cb, sb, mb + sb * (sb / jnp.maximum(cb, 1.0))

    def keep_local(c, groups):
        def one(p, _):
            for q, value in enumerate(gather(c, z * PATCH_DEV + p, groups)):
                local[c, p, q] = value
            return 0
        lax.fori_loop(0, PATCH_DEV, one, 0)

    def finish(c):
        lanes = pl.ds(pl.multiple_of(c // slabs * width, width), width)
        hub = jnp.logical_xor(inner, swapped(c))

        @pl.when(hub)
        def _():
            sums_arrived(c, 1)

        @pl.when(jnp.logical_not(hub))
        def _():
            sums_arrived(c, 2)
            for p in range(PATCH_DEV):
                for q, value in enumerate(total(c, half, p)):
                    local[c, p, q] = local[c, p, q] + value

        for p in range(PATCH_DEV):
            cf, sf, qf, cb, sb, qb = [local[c, p, q] + value for q, value in enumerate(total(c, 1 - half, p))]
            mean = sf / jnp.maximum(cf, 1.0)
            shift = sb - mean * cb
            square = qb - mean * sb - mean * shift
            step = shift / jnp.maximum(cb, 1.0)
            first_var = (qf - sf * mean) / jnp.maximum(cf - 1.0, 1.0)
            final_var = (square - shift * step) / jnp.maximum(cb - 1.0, 1.0)
            for h in range(slabs):
                @pl.when(c % slabs == h)
                def _(h=h, p=p, values=(mean, mean + step, first_var, final_var)):
                    for q, value in enumerate(values):
                        out_ref[q // 2, q % 2, p, h * slab:(h + 1) * slab, lanes] = value

    def other_tables():
        arrived(held_s.at[pl.ds(0, depth)], r_s.at[1])
        more = pltpu.make_async_copy(held_s.at[pl.ds(depth, depth)], tables.at[1], s_l.at[1])
        more.start()
        more.wait()

    @pl.when(outer)
    def _():
        def leaf(i, _):
            c = chunk(i)
            row_arrived(c)
            send_onward(c)

            @pl.when(jnp.logical_and(i >= LEAD - 1, i + 1 < chain))
            def _():
                send_direct(chunk(i + 1))
            return 0

        lax.fori_loop(0, chain, leaf, 0)
        row_tables()
        other_tables()

        def own(i, _):
            c = chunk(i)
            stage(c, 0, *mine)
            keep_local(c, 1)
            return 0

        lax.fori_loop(0, chain, own, 0)

        def turned(c, _):
            row_arrived(c)
            raw_arrived(c)
            stage(c, 0, *mine)
            stage(c, 1, *theirs)
            send_sums(c, 1, across, 2)
            send_sums(c, 0, beyond, 2)
            send_sums(c, 2, mate, 1)
            keep_local(c, 2)
            return 0

        lax.fori_loop(first, first + SWAP, turned, 0)

    @pl.when(inner)
    def _():
        row_tables()
        other_tables()

        def hub(i, _):
            c = chunk(i)

            row_arrived(c)

            @pl.when(i == TURN)
            def _():
                def turned(q, _):
                    row_arrived(q)
                    send_onward(q)
                    stage(q, 0, *mine)
                    keep_local(q, 1)
                    return 0
                lax.fori_loop(first, first + SWAP, turned, 0)

            stage(c, 0, *mine)
            send_sums(c, 2, mate, 1)
            raw_arrived(c)
            stage(c, 1, *theirs)
            send_sums(c, 0, beyond, 2)
            send_sums(c, 1, across, 2)
            keep_local(c, 2)

            @pl.when(i >= LAG)
            def _():
                finish(chunk(i - LAG))
            return 0

        lax.fori_loop(0, chain, hub, 0)

    def close(i, _):
        @pl.when(jnp.logical_or(outer, i >= chain - LAG))
        def _():
            turn = jnp.logical_and(i >= chain - 1, i < parts - 1)
            finish(jnp.where(turn, i - chain + 1 + first, chunk(jnp.minimum(i, chain - 1))))
        return 0

    lax.fori_loop(0, parts, close, 0)

    left(out_t.at[:, pl.ds(0, depth - 1)], s_x.at[0])
    left(out_b.at[:, pl.ds(0, depth - 1)], s_x.at[1])

    left(held_s.at[pl.ds(0, 2 * depth - 1)], s_s.at[0])

    def all_left(sent, bands_sent, summed):
        left(out_t.at[pl.ds(0, sent)], s_y.at[0])
        left(out_b.at[pl.ds(0, bands_sent)], s_y.at[1])
        left(far32.at[pl.ds(0, summed)], s_y.at[2])
        left(far16.at[pl.ds(0, summed)], s_y.at[3])

    @pl.when(outer)
    def _():
        all_left(chain, bands, SWAP)

    @pl.when(inner)
    def _():
        all_left(SWAP, 1, chain)


def split(both_ref, mean_hbm, var_hbm, sems):
    copies = [pltpu.make_async_copy(both_ref.at[q], out, sems.at[q]) for q, out in enumerate((mean_hbm, var_hbm))]
    for copy in copies:
        copy.start()
    for copy in copies:
        copy.wait()


def per_device(sky, depth, visit_tiles, warp_matrix, flux_scale, patch_lists, clip_bits):
    visits, own, rows, columns = visit_tiles.shape
    entries = visits * own
    patches = PATCH_DEV * sky
    devices = sky * depth
    share = rows // depth
    smem, vmem = pl.BlockSpec(memory_space=pltpu.SMEM), pl.BlockSpec(memory_space=pltpu.VMEM)
    hbm = pl.BlockSpec(memory_space=pltpu.HBM)
    out = jax.ShapeDtypeStruct((2, PATCH_DEV, share, columns), jnp.float32)
    if sky == 4 and depth == 4 and share == 16:
        width = 128
        slab = SLAB
        bands = columns // width
        parts = bands * (share // slab)
        long = -(-patches * CAPACITY // 128) * 128
        blocks = (parts, depth, entries, slab, width)
        flags = (bands, depth, entries, 1, width)
        work = (2, depth, entries + 1)
        dma = pltpu.SemaphoreType.DMA
        both = pl.pallas_call(
            functools.partial(folded, depth),
            out_shape=jax.ShapeDtypeStruct((2,) + out.shape, jnp.float32),
            in_specs=[hbm] * 5,
            out_specs=vmem,
            scratch_shapes=[
                pltpu.SMEM((visits,), jnp.float32),
                pltpu.SMEM((visits, own), jnp.int32),
                pltpu.VMEM((visits, own * rows, columns), jnp.bfloat16),
                pltpu.VMEM((bands, visits, columns, width), jnp.bfloat16),
                pltpu.VMEM((entries, rows // 16, columns), jnp.int32),
                dma((bands + 4,)),
                pltpu.VMEM(blocks, jnp.bfloat16), pltpu.VMEM(flags, jnp.int32),
                pltpu.VMEM(blocks, jnp.bfloat16), pltpu.VMEM(flags, jnp.int32),
                pltpu.VMEM(blocks, jnp.bfloat16), pltpu.VMEM(flags, jnp.int32),
                pltpu.VMEM((1, long), jnp.int32), pltpu.VMEM((2 * depth, 1, long), jnp.int32),
                pltpu.VMEM((parts, 3, PATCH_DEV, slab, width), jnp.float32),
                pltpu.VMEM((parts, 3, PATCH_DEV, 5, slab, width), jnp.bfloat16),
                pltpu.VMEM((parts, 2, PATCH_DEV, slab, width), jnp.float32),
                pltpu.VMEM((parts, 2, PATCH_DEV, 5, slab, width), jnp.bfloat16),
                pltpu.SMEM((2, depth, 1, long), jnp.int32),
                pltpu.VMEM((parts, PATCH_DEV, 6, slab, width), jnp.float32),
                pltpu.VMEM(work + blocks[3:], jnp.bfloat16), pltpu.VMEM(work + flags[3:], jnp.int32),
                dma((2,)), dma((4,)), dma((1,)), dma((parts,)), dma((parts,)), dma((2,)), dma((parts,)), dma((2,)),
            ],
            compiler_params=pltpu.CompilerParams(
                collective_id=0, has_side_effects=True, vmem_limit_bytes=24 * 1024 * 1024
            ),
        )(*[pltpu.with_memory_space_constraint(x, pltpu.HBM) for x in (
            flux_scale, patch_lists, visit_tiles.reshape(visits, own * rows, columns), warp_matrix,
            clip_bits.reshape(entries, rows // 16, columns))])
        return pl.pallas_call(
            split, out_shape=(out, out), in_specs=[vmem], out_specs=(hbm, hbm),
            scratch_shapes=[dma((2,))],
            compiler_params=pltpu.CompilerParams(vmem_limit_bytes=8 * 1024 * 1024),
        )(both)
    targets = patch_lists.reshape(entries)
    number = jnp.arange(entries, dtype=jnp.int32)
    same = (targets[:, None] == targets[None, :]) & (number[None, :] < number[:, None])
    rank = jnp.sum(same.astype(jnp.int32), axis=1)
    slot = targets * CAPACITY + rank
    source = jnp.min(
        jnp.where(slot[None, :] == jnp.arange(patches * CAPACITY, dtype=jnp.int32)[:, None], number[None, :], entries),
        axis=1,
    )
    return pl.pallas_call(
        functools.partial(kernel, sky, depth),
        out_shape=(out, out),
        in_specs=[smem, smem, vmem, vmem, vmem],
        out_specs=(vmem, vmem),
        scratch_shapes=[
            pltpu.VMEM((entries, rows, columns), jnp.bfloat16),
            pltpu.VMEM((devices, SLOTS, share, columns), jnp.bfloat16),
            pltpu.VMEM((devices, SLOTS, share // 16, columns), jnp.int32),
            pltpu.VMEM((devices, SLOTS, share, columns), jnp.bfloat16),
            pltpu.VMEM((devices, SLOTS, share // 16, columns), jnp.int32),
            pltpu.VMEM((PATCH_DEV, 6, share, columns), jnp.float32),
        ] + [pltpu.SemaphoreType.DMA((devices,))] * 4,
        compiler_params=pltpu.CompilerParams(
            collective_id=0, has_side_effects=True, vmem_limit_bytes=67043328 - 1048576
        ),
    )(flux_scale, source, visit_tiles.reshape(visits, own * rows, columns), warp_matrix,
      clip_bits.reshape(entries, rows // 16, columns))


def solution(mesh):
    whole = ("tracts", "sky", "depth")
    placed = (P(whole, None, None, None), P(whole, None, None), P(whole), P(whole, None), P(whole, None, None, None))
    outs = P(None, ("tracts", "sky"), "depth", None)
    return jax.shard_map(
        functools.partial(per_device, mesh.shape["sky"], mesh.shape["depth"]),
        mesh=mesh,
        in_specs=placed,
        out_specs=(outs, outs),
        check_vma=False,
    )
```

```python
import functools

import jax
import jax.numpy as jnp
from jax import lax
from jax.experimental import pallas as pl
from jax.experimental.pallas import tpu as pltpu
from jax.sharding import PartitionSpec as P

PATCH_DEV = 4
CAPACITY = 2
SLOTS = PATCH_DEV * CAPACITY
MESH = pl.DeviceIdType.MESH
STEP = 4
LAG = 5
LEAD = 5
PRE = 5
SLAB = 4
PIECES = 8
SWAP = 3
TURN = 8


def kernel(sky, depth, scale_ref, src_ref, tiles_ref, matrix_ref, bits_ref, mean_ref, var_ref,
           warped, send_t, send_b, recv_t, recv_b, acc, st, sb, rt, rb):
    z, d = lax.axis_index("sky"), lax.axis_index("depth")
    me = z * depth + d
    devices = sky * depth
    visits, entries_rows, columns = tiles_ref.shape
    entries, rows, _ = warped.shape
    share = rows // depth

    def place(j):
        return lax.div(lax.rem(me + j, devices), depth), lax.rem(lax.rem(me + j, devices), depth)

    barrier = pltpu.get_barrier_semaphore()

    def greet(j, _):
        zz, dd = place(j)
        pl.semaphore_signal(barrier, inc=1, device_id={"sky": zz, "depth": dd}, device_id_type=MESH)
        return 0

    lax.fori_loop(1, devices, greet, 0)

    per_visit = entries // visits
    for v in range(visits):
        def warp(i, _, v=v):
            start = pl.multiple_of(i * STEP * rows, STEP * rows)
            product = jnp.dot(tiles_ref[v, pl.ds(start, STEP * rows), :], matrix_ref[v],
                              preferred_element_type=jnp.float32) * scale_ref[v]
            warped[pl.ds(v * per_visit + i * STEP, STEP)] = product.astype(jnp.bfloat16).reshape(STEP, rows, columns)
            return 0
        lax.fori_loop(0, per_visit // STEP, warp, 0)

    pl.semaphore_wait(barrier, devices - 1)

    def copies(zz, dd, there, mine):
        to = {"sky": zz, "depth": dd}
        return (
            pltpu.make_async_remote_copy(src_ref=send_t.at[there], dst_ref=recv_t.at[mine], send_sem=st.at[there],
                                         recv_sem=rt.at[mine], device_id=to, device_id_type=MESH),
            pltpu.make_async_remote_copy(src_ref=send_b.at[there], dst_ref=recv_b.at[mine], send_sem=sb.at[there],
                                         recv_sem=rb.at[mine], device_id=to, device_id_type=MESH),
        )

    def post(jj, _):
        zz = lax.rem(z + sky // 2 + jj, sky)

        def fill(s, _):
            e = src_ref[zz * SLOTS + s]
            valid = (e < entries).astype(jnp.int32)
            e = jnp.minimum(e, entries - 1)
            block = warped[e]
            flags = bits_ref[e] * valid
            for dd in range(depth):
                send_t[zz * depth + dd, s] = block[dd * share:(dd + 1) * share]
                send_b[zz * depth + dd, s] = flags[dd * (share // 16):(dd + 1) * (share // 16)]
            return 0

        lax.fori_loop(0, SLOTS, fill, 0)

        def start(k, _):
            dd = lax.rem(d + k, depth)
            there = zz * depth + dd

            @pl.when(there != me)
            def _():
                for c in copies(zz, dd, there, me):
                    c.start()
            return 0

        lax.fori_loop(0, depth, start, 0)
        return 0

    lax.fori_loop(0, sky, post, 0)

    acc[...] = jnp.zeros_like(acc)
    position = lax.rem(lax.broadcasted_iota(jnp.int32, (share, columns), 0), 16)

    def add(tiles, flags, source):
        for p in range(PATCH_DEV):
            sums = [acc[p, q] for q in range(6)]
            for c in range(CAPACITY):
                w = tiles[source, p * CAPACITY + c].astype(jnp.float32)
                packed = flags[source, p * CAPACITY + c]
                packed = jnp.broadcast_to(packed[:, None, :], (share // 16, 16, columns)).reshape(share, columns)
                shifted = lax.shift_right_logical(packed, position)
                first = (shifted & 1).astype(jnp.float32)
                both = first * (lax.shift_right_logical(shifted, 16) & 1).astype(jnp.float32)
                fw, bw = first * w, both * w
                for q, term in enumerate((first, fw, fw * w, both, bw, bw * w)):
                    sums[q] = sums[q] + term
            for q in range(6):
                acc[p, q] = sums[q]

    add(send_t, send_b, me)

    def take(jj, _):
        zz = lax.rem(z - sky // 2 - jj + 2 * sky, sky)

        def one(k, _):
            dd = lax.rem(d - k + depth, depth)
            there = zz * depth + dd

            @pl.when(there != me)
            def _():
                for c in copies(zz, dd, there, there):
                    c.wait_recv()
                add(recv_t, recv_b, there)
            return 0

        lax.fori_loop(0, depth, one, 0)
        return 0

    lax.fori_loop(0, sky, take, 0)

    for p in range(PATCH_DEV):
        cf, sf, qf, cb, sb_, qb = [acc[p, q] for q in range(6)]
        mean = sf / jnp.maximum(cf, 1.0)
        shift = sb_ - mean * cb
        square = qb - mean * sb_ - mean * shift
        step = shift / jnp.maximum(cb, 1.0)
        mean_ref[0, p] = mean
        mean_ref[1, p] = mean + step
        var_ref[0, p] = (qf - sf * mean) / jnp.maximum(cf - 1.0, 1.0)
        var_ref[1, p] = (square - shift * step) / jnp.maximum(cb - 1.0, 1.0)

    def drain(j, _):
        zz, dd = place(j)
        for c in copies(zz, dd, zz * depth + dd, me):
            c.wait_send()
        return 0

    lax.fori_loop(1, devices, drain, 0)


def folded(depth, scale_hbm, lists_hbm, tiles_hbm, matrix_hbm, bits_hbm, out_ref,
           scale_ref, lists_ref, tiles_ref, matrix_ref, bits_ref, s_in,
           out_t, out_b, row_t, row_b, raw_t, raw_b, own_s, held_s, far32, far16, got32, got16, tables, local, part,
           work_t, work_b, s_x, s_y, s_s, r_x, r_y, r_s, r_g, s_l):
    z, d = lax.axis_index("sky"), lax.axis_index("depth")
    half = z // 2
    rem = z - 2 * half
    inner, outer = rem != half, rem == half
    mate = 2 * half + 1 - rem
    across, beyond = 3 - z, 3 - mate
    base = d // 2 * 2
    other = depth - 2 - base
    twin = 2 * base + 1 - d
    parts, _, entries, slab, width = out_t.shape
    visits, entries_rows, columns = tiles_ref.shape
    per_visit = entries // visits
    rows = entries_rows // per_visit
    share = rows // depth
    slabs = share // slab
    long = own_s.shape[1]

    bands = matrix_ref.shape[0]
    first = bands // 2 * slabs + slabs - SWAP
    chain = parts - SWAP

    def chunk(i):
        return i + jnp.where(i >= first, SWAP, 0)

    def swapped(c):
        return jnp.logical_and(c >= first, c < first + SWAP)

    def fresh(c):
        return jnp.logical_or(c % slabs == 0, c == first)

    tiles_in = pltpu.make_async_copy(tiles_hbm, tiles_ref, s_in.at[bands])
    bits_in = pltpu.make_async_copy(bits_hbm, bits_ref, s_in.at[bands + 1])
    scale_in = pltpu.make_async_copy(scale_hbm, scale_ref, s_in.at[bands + 2])
    lists_in = pltpu.make_async_copy(lists_hbm, lists_ref, s_in.at[bands + 3])

    def matrix_in(band):
        lanes = pl.ds(band * width, width)
        return pltpu.make_async_copy(matrix_hbm.at[:, :, lanes], matrix_ref.at[band], s_in.at[band])

    barrier = pltpu.get_barrier_semaphore()
    for k in range(1, depth):
        pl.semaphore_signal(barrier, inc=1, device_id={"depth": lax.rem(d + k, depth)}, device_id_type=MESH)
    for k in range(depth):
        pl.semaphore_signal(barrier, inc=1, device_id={"sky": mate, "depth": k}, device_id_type=MESH)
    for far in (across, beyond):
        pl.semaphore_signal(barrier, inc=1, device_id={"sky": far}, device_id_type=MESH)

    tiles_in.start()
    matrix_in(0).start()
    lists_in.start()
    scale_in.start()
    bits_in.start()

    def remote(src, dst, send, recv, to):
        return pltpu.make_async_remote_copy(src_ref=src, dst_ref=dst, send_sem=send, recv_sem=recv, device_id=to,
                                            device_id_type=MESH)

    def to_row(c, there):
        return remote(out_t.at[c, there], row_t.at[c, d], s_x.at[0], r_x.at[c], {"depth": there})

    def flags_to_row(b, there):
        return remote(out_b.at[b, there], row_b.at[b, d], s_x.at[1], r_x.at[slabs * b], {"depth": there})

    def table_to_row(there):
        return remote(own_s, held_s.at[d], s_s.at[0], r_s.at[0], {"depth": there})

    def table_to_mates(there):
        return remote(own_s, held_s.at[depth + d], s_s.at[0], r_s.at[1], {"sky": mate, "depth": there})

    def direct(c, there):
        to = {"sky": mate, "depth": there}
        return remote(out_t.at[c, there], raw_t.at[c, d], s_y.at[0], r_y.at[c], to)

    def flags_direct(c, there):
        to = {"sky": mate, "depth": there}
        b = c // slabs
        return remote(out_b.at[b, there], raw_b.at[b, d], s_y.at[1], r_y.at[c], to)

    def onward(c):
        pair = pl.ds(other, 2)
        return remote(row_t.at[c, pair], raw_t.at[c, pair], s_y.at[0], r_y.at[c], {"sky": mate})

    def flags_onward(c):
        b, pair = c // slabs, pl.ds(other, 2)
        return remote(row_b.at[b, pair], raw_b.at[b, pair], s_y.at[1], r_y.at[c], {"sky": mate})

    def sums_to(c, t, where, slot):
        to = {"sky": where}
        return (remote(far32.at[c, t], got32.at[c, slot], s_y.at[2], r_g.at[c], to),
                remote(far16.at[c, t], got16.at[c, slot], s_y.at[3], r_g.at[c], to))

    def arrived(ref, sem):
        remote(ref, ref, s_x.at[0], sem, {"sky": mate}).wait_recv()

    def left(ref, sem):
        remote(ref, ref, sem, r_s.at[0], {"sky": mate}).wait_send()

    def volume(tiles):
        a, b, k = next((a, b, k) for a in range(1, parts + 1) for b in range(1, depth + 1)
                       for k in range(1, entries + 1) if a * b * k == tiles)
        return out_t.at[pl.ds(0, a), pl.ds(0, b), pl.ds(0, k)]

    def blocks_arrived(c, flags, sem, count):
        flag_tiles = 2 * entries // slab

        @pl.when(flags)
        def _():
            arrived(volume(count * (entries + flag_tiles)), sem.at[c])

        @pl.when(jnp.logical_not(flags))
        def _():
            arrived(volume(count * entries), sem.at[c])

    def row_arrived(c):
        blocks_arrived(c, c % slabs == 0, r_x, depth - 1)

    def raw_arrived(c):
        blocks_arrived(c, fresh(c), r_y, depth)

    def sums_arrived(c, slots):
        arrived(volume(slots * PATCH_DEV * 7), r_g.at[c])

    position = lax.broadcasted_iota(jnp.int32, (slab, width), 0)
    for which in range(2):
        for dd in range(depth):
            work_t[which, dd, entries] = jnp.zeros((slab, width), jnp.bfloat16)
            work_b[which, dd, entries] = jnp.zeros((1, width), jnp.int32)

    lists_in.wait()
    for band in range(1, bands):
        matrix_in(band).start()
    lane = lax.broadcasted_iota(jnp.int32, (1, long), 1)
    table = jnp.full((1, long), entries, jnp.int32)
    targets = [lists_ref[v, k] for v in range(visits) for k in range(per_visit)]
    for e in range(entries):
        rank = jnp.int32(0)
        for f in range(e // per_visit * per_visit):
            rank = rank + (targets[e] == targets[f]).astype(jnp.int32)
        table = jnp.where(lane == targets[e] * CAPACITY + rank, e, table)
    own_s[...] = table
    held_s[d] = table

    def stage(c, which, tiles, flags):
        work_t[which, :, :entries] = tiles[c]
        work_b[which, :, :entries] = flags[c // slabs]

    def gather(c, patch, groups, start=0):
        place = position + (c % slabs) * slab
        sums = [jnp.zeros((slab, width), jnp.float32)] * 6
        for which in range(start, groups):
            for dd in range(depth):
                for k in range(CAPACITY):
                    e = tables[which, dd, 0, patch * CAPACITY + k]
                    w = work_t[which, dd, e].astype(jnp.float32)
                    packed = jnp.broadcast_to(work_b[which, dd, e], (slab, width))
                    shifted = lax.shift_right_logical(packed, place)
                    first = (shifted & 1).astype(jnp.float32)
                    both = first * (lax.shift_right_logical(shifted, 16) & 1).astype(jnp.float32)
                    fw, bw = first * w, both * w
                    sums = [a + b for a, b in zip(sums, (first, fw, fw * w, both, bw, bw * w))]
        return sums

    def keep_part(c, t, where):
        def one(p, _):
            for q, value in enumerate(gather(c, where * PATCH_DEV + p, 1)):
                part[t, p, q] = value
            return 0
        lax.fori_loop(0, PATCH_DEV, one, 0)

    def send_sums(c, t, where, groups):
        def one(p, _):
            sums = gather(c, where * PATCH_DEV + p, groups, groups - 1)
            if groups == 2:
                sums = [part[t, p, q] + value for q, value in enumerate(sums)]
            cf, sf, qf, cb, sb, qb = sums
            mean = sf / jnp.maximum(cf, 1.0)
            far32[c, t, p] = sf
            packed = (cf, cb, qf - sf * mean, sb - mean * cb, qb - sb * (sb / jnp.maximum(cb, 1.0)))
            for q, value in enumerate(packed):
                far16[c, t, p, q] = value.astype(jnp.bfloat16)
            return 0
        lax.fori_loop(0, PATCH_DEV, one, 0)
        for copy in sums_to(c, t, where, half):
            copy.start()

    def send_direct(c):
        @pl.when(fresh(c))
        def _():
            for j in range(2):
                flags_direct(c, base + j).start()
        for j in range(2):
            direct(c, base + j).start()

    def send_onward(c):
        @pl.when(fresh(c))
        def _():
            flags_onward(c).start()
        onward(c).start()

    def warp(column, _):
        lanes = pl.ds(pl.multiple_of(column * width, width), width)
        for band in range(bands):
            @pl.when(column == band)
            def _(band=band):
                matrix_in(band).wait()
        for v in range(visits):
            product = jnp.dot(tiles_ref[v], matrix_ref[column, v], preferred_element_type=jnp.float32)
            block = (product * scale_ref[v]).reshape(per_visit, depth, slabs, slab, width)
            for dd in range(depth):
                for h in range(slabs):
                    out_t[column * slabs + h, dd, v * per_visit:(v + 1) * per_visit] = block[:, dd, h].astype(jnp.bfloat16)
        for dd in range(depth):
            out_b[column, dd] = bits_ref[:, dd:dd + 1, lanes]
        row_b[column, d] = out_b[column, d]
        for h in range(slabs):
            row_t[column * slabs + h, d] = out_t[column * slabs + h, d]

        @pl.when(column == 0)
        def _():
            pl.semaphore_wait(barrier, 2 * depth + 1)

        for h in range(slabs):
            for there in (other, other + 1, twin):
                if h == 0:
                    flags_to_row(column, there).start()
                to_row(column * slabs + h, there).start()

            c = column * slabs + h

            @pl.when(jnp.logical_or(jnp.logical_and(outer, c < PRE), jnp.logical_and(inner, swapped(c))))
            def _(c=c):
                send_direct(c)

            if h == 0:
                @pl.when(column == 0)
                def _():
                    for k in range(1, depth):
                        table_to_row(lax.rem(d + k, depth)).start()
                    for k in range(depth):
                        table_to_mates(k).start()
        return 0

    tiles_in.wait()
    scale_in.wait()
    bits_in.wait()
    lax.fori_loop(0, bands, warp, 0)
    mine, theirs = (row_t, row_b), (raw_t, raw_b)

    def row_tables():
        arrived(held_s.at[pl.ds(0, depth - 1)], r_s.at[0])
        held = pltpu.make_async_copy(held_s.at[pl.ds(0, depth)], tables.at[0], s_l.at[0])
        held.start()
        held.wait()

    def total(c, slot, p):
        sf = got32[c, slot, p]
        cf, cb, mf, shift, mb = [got16[c, slot, p, q].astype(jnp.float32) for q in range(5)]
        mean = sf / jnp.maximum(cf, 1.0)
        sb = shift + mean * cb
        return cf, sf, mf + sf * mean, cb, sb, mb + sb * (sb / jnp.maximum(cb, 1.0))

    def keep_local(c, groups):
        def one(p, _):
            for q, value in enumerate(gather(c, z * PATCH_DEV + p, groups)):
                local[c, p, q] = value
            return 0
        lax.fori_loop(0, PATCH_DEV, one, 0)

    def finish(c):
        lanes = pl.ds(pl.multiple_of(c // slabs * width, width), width)
        hub = jnp.logical_xor(inner, swapped(c))

        @pl.when(hub)
        def _():
            sums_arrived(c, 1)

        @pl.when(jnp.logical_not(hub))
        def _():
            sums_arrived(c, 2)
            for p in range(PATCH_DEV):
                for q, value in enumerate(total(c, half, p)):
                    local[c, p, q] = local[c, p, q] + value

        for p in range(PATCH_DEV):
            cf, sf, qf, cb, sb, qb = [local[c, p, q] + value for q, value in enumerate(total(c, 1 - half, p))]
            mean = sf / jnp.maximum(cf, 1.0)
            shift = sb - mean * cb
            square = qb - mean * sb - mean * shift
            step = shift / jnp.maximum(cb, 1.0)
            first_var = (qf - sf * mean) / jnp.maximum(cf - 1.0, 1.0)
            final_var = (square - shift * step) / jnp.maximum(cb - 1.0, 1.0)
            for h in range(slabs):
                @pl.when(c % slabs == h)
                def _(h=h, p=p, values=(mean, mean + step, first_var, final_var)):
                    for q, value in enumerate(values):
                        out_ref[q // 2, q % 2, p, h * slab:(h + 1) * slab, lanes] = value

    def other_tables():
        arrived(held_s.at[pl.ds(0, depth)], r_s.at[1])
        more = pltpu.make_async_copy(held_s.at[pl.ds(depth, depth)], tables.at[1], s_l.at[1])
        more.start()
        more.wait()

    @pl.when(outer)
    def _():
        def leaf(i, _):
            c = chunk(i)
            row_arrived(c)
            send_onward(c)

            @pl.when(i < LEAD - PRE)
            def _():
                send_direct(chunk(i + PRE))

            @pl.when(jnp.logical_and(i >= LEAD - 1, i + 1 < chain))
            def _():
                send_direct(chunk(i + 1))
            return 0

        lax.fori_loop(0, chain, leaf, 0)
        row_tables()
        other_tables()

        def own(i, _):
            c = chunk(i)
            stage(c, 0, *mine)
            keep_local(c, 1)
            return 0

        lax.fori_loop(0, chain, own, 0)

        def turned(c, _):
            row_arrived(c)
            raw_arrived(c)
            stage(c, 0, *mine)
            keep_part(c, 0, beyond)
            keep_part(c, 1, across)
            stage(c, 1, *theirs)
            send_sums(c, 1, across, 2)
            send_sums(c, 0, beyond, 2)
            send_sums(c, 2, mate, 1)
            keep_local(c, 2)
            return 0

        lax.fori_loop(first, first + SWAP, turned, 0)

    @pl.when(inner)
    def _():
        row_tables()
        other_tables()

        def hub(i, _):
            c = chunk(i)

            row_arrived(c)

            @pl.when(i == TURN)
            def _():
                def turned(q, _):
                    row_arrived(q)
                    send_onward(q)
                    stage(q, 0, *mine)
                    keep_local(q, 1)
                    return 0
                lax.fori_loop(first, first + SWAP, turned, 0)

            stage(c, 0, *mine)
            send_sums(c, 2, mate, 1)
            keep_part(c, 0, beyond)
            keep_part(c, 1, across)
            raw_arrived(c)
            stage(c, 1, *theirs)
            send_sums(c, 0, beyond, 2)
            send_sums(c, 1, across, 2)
            keep_local(c, 2)

            @pl.when(i >= LAG)
            def _():
                finish(chunk(i - LAG))
            return 0

        lax.fori_loop(0, chain, hub, 0)

    def close(i, _):
        @pl.when(jnp.logical_or(outer, i >= chain - LAG))
        def _():
            turn = jnp.logical_and(i >= chain - 1, i < parts - 1)
            finish(jnp.where(turn, i - chain + 1 + first, chunk(jnp.minimum(i, chain - 1))))
        return 0

    lax.fori_loop(0, parts, close, 0)

    left(out_t.at[:, pl.ds(0, depth - 1)], s_x.at[0])
    left(out_b.at[:, pl.ds(0, depth - 1)], s_x.at[1])

    left(held_s.at[pl.ds(0, 2 * depth - 1)], s_s.at[0])

    def all_left(sent, bands_sent, summed):
        left(out_t.at[pl.ds(0, sent)], s_y.at[0])
        left(out_b.at[pl.ds(0, bands_sent)], s_y.at[1])
        left(far32.at[pl.ds(0, summed)], s_y.at[2])
        left(far16.at[pl.ds(0, summed)], s_y.at[3])

    @pl.when(outer)
    def _():
        all_left(chain, bands, SWAP)

    @pl.when(inner)
    def _():
        all_left(SWAP, 1, chain)


def split(both_ref, mean_hbm, var_hbm, sems):
    outs = (mean_hbm, var_hbm)
    steps, patches = mean_hbm.shape[:2]
    pieces = PIECES // steps
    each = patches // pieces
    for t in range(steps):
        for p in range(pieces):
            part = pl.ds(p * each, each)
            for q, out in enumerate(outs):
                pltpu.make_async_copy(both_ref.at[q, t, part], out.at[t, part], sems.at[q]).start()
    for q, out in enumerate(outs):
        pltpu.make_async_copy(both_ref.at[q], out, sems.at[q]).wait()


def per_device(sky, depth, visit_tiles, warp_matrix, flux_scale, patch_lists, clip_bits):
    visits, own, rows, columns = visit_tiles.shape
    entries = visits * own
    patches = PATCH_DEV * sky
    devices = sky * depth
    share = rows // depth
    smem, vmem = pl.BlockSpec(memory_space=pltpu.SMEM), pl.BlockSpec(memory_space=pltpu.VMEM)
    hbm = pl.BlockSpec(memory_space=pltpu.HBM)
    out = jax.ShapeDtypeStruct((2, PATCH_DEV, share, columns), jnp.float32)
    if sky == 4 and depth == 4 and share == 16:
        width = 128
        slab = SLAB
        bands = columns // width
        parts = bands * (share // slab)
        long = -(-patches * CAPACITY // 128) * 128
        blocks = (parts, depth, entries, slab, width)
        flags = (bands, depth, entries, 1, width)
        work = (2, depth, entries + 1)
        dma = pltpu.SemaphoreType.DMA
        both = pl.pallas_call(
            functools.partial(folded, depth),
            out_shape=jax.ShapeDtypeStruct((2,) + out.shape, jnp.float32),
            in_specs=[hbm] * 5,
            out_specs=vmem,
            scratch_shapes=[
                pltpu.SMEM((visits,), jnp.float32),
                pltpu.SMEM((visits, own), jnp.int32),
                pltpu.VMEM((visits, own * rows, columns), jnp.bfloat16),
                pltpu.VMEM((bands, visits, columns, width), jnp.bfloat16),
                pltpu.VMEM((entries, rows // 16, columns), jnp.int32),
                dma((bands + 4,)),
                pltpu.VMEM(blocks, jnp.bfloat16), pltpu.VMEM(flags, jnp.int32),
                pltpu.VMEM(blocks, jnp.bfloat16), pltpu.VMEM(flags, jnp.int32),
                pltpu.VMEM(blocks, jnp.bfloat16), pltpu.VMEM(flags, jnp.int32),
                pltpu.VMEM((1, long), jnp.int32), pltpu.VMEM((2 * depth, 1, long), jnp.int32),
                pltpu.VMEM((parts, 3, PATCH_DEV, slab, width), jnp.float32),
                pltpu.VMEM((parts, 3, PATCH_DEV, 5, slab, width), jnp.bfloat16),
                pltpu.VMEM((parts, 2, PATCH_DEV, slab, width), jnp.float32),
                pltpu.VMEM((parts, 2, PATCH_DEV, 5, slab, width), jnp.bfloat16),
                pltpu.SMEM((2, depth, 1, long), jnp.int32),
                pltpu.VMEM((parts, PATCH_DEV, 6, slab, width), jnp.float32),
                pltpu.VMEM((2, PATCH_DEV, 6, slab, width), jnp.float32),
                pltpu.VMEM(work + blocks[3:], jnp.bfloat16), pltpu.VMEM(work + flags[3:], jnp.int32),
                dma((2,)), dma((4,)), dma((1,)), dma((parts,)), dma((parts,)), dma((2,)), dma((parts,)), dma((2,)),
            ],
            compiler_params=pltpu.CompilerParams(
                collective_id=0, has_side_effects=True, vmem_limit_bytes=24 * 1024 * 1024
            ),
        )(*[pltpu.with_memory_space_constraint(x, pltpu.HBM) for x in (
            flux_scale, patch_lists, visit_tiles.reshape(visits, own * rows, columns), warp_matrix,
            clip_bits.reshape(entries, rows // 16, columns))])
        return pl.pallas_call(
            split, out_shape=(out, out), in_specs=[vmem], out_specs=(hbm, hbm),
            scratch_shapes=[dma((2,))],
            compiler_params=pltpu.CompilerParams(vmem_limit_bytes=8 * 1024 * 1024),
        )(both)
    targets = patch_lists.reshape(entries)
    number = jnp.arange(entries, dtype=jnp.int32)
    same = (targets[:, None] == targets[None, :]) & (number[None, :] < number[:, None])
    rank = jnp.sum(same.astype(jnp.int32), axis=1)
    slot = targets * CAPACITY + rank
    source = jnp.min(
        jnp.where(slot[None, :] == jnp.arange(patches * CAPACITY, dtype=jnp.int32)[:, None], number[None, :], entries),
        axis=1,
    )
    return pl.pallas_call(
        functools.partial(kernel, sky, depth),
        out_shape=(out, out),
        in_specs=[smem, smem, vmem, vmem, vmem],
        out_specs=(vmem, vmem),
        scratch_shapes=[
            pltpu.VMEM((entries, rows, columns), jnp.bfloat16),
            pltpu.VMEM((devices, SLOTS, share, columns), jnp.bfloat16),
            pltpu.VMEM((devices, SLOTS, share // 16, columns), jnp.int32),
            pltpu.VMEM((devices, SLOTS, share, columns), jnp.bfloat16),
            pltpu.VMEM((devices, SLOTS, share // 16, columns), jnp.int32),
            pltpu.VMEM((PATCH_DEV, 6, share, columns), jnp.float32),
        ] + [pltpu.SemaphoreType.DMA((devices,))] * 4,
        compiler_params=pltpu.CompilerParams(
            collective_id=0, has_side_effects=True, vmem_limit_bytes=67043328 - 1048576
        ),
    )(flux_scale, source, visit_tiles.reshape(visits, own * rows, columns), warp_matrix,
      clip_bits.reshape(entries, rows // 16, columns))


def solution(mesh):
    whole = ("tracts", "sky", "depth")
    placed = (P(whole, None, None, None), P(whole, None, None), P(whole), P(whole, None), P(whole, None, None, None))
    outs = P(None, ("tracts", "sky"), "depth", None)
    return jax.shard_map(
        functools.partial(per_device, mesh.shape["sky"], mesh.shape["depth"]),
        mesh=mesh,
        in_specs=placed,
        out_specs=(outs, outs),
        check_vma=False,
    )
```

```python
import functools

import jax
import jax.numpy as jnp
from jax import lax
from jax.experimental import pallas as pl
from jax.experimental.pallas import tpu as pltpu
from jax.sharding import PartitionSpec as P

PATCH_DEV = 4
CAPACITY = 2
SLOTS = PATCH_DEV * CAPACITY
MESH = pl.DeviceIdType.MESH
STEP = 4
LAG = 5
LEAD = 5
PRE = 5
SLAB = 4
PIECES = 8
SWAP = 3
TURN = 8


def kernel(sky, depth, scale_ref, src_ref, tiles_ref, matrix_ref, bits_ref, mean_ref, var_ref,
           warped, send_t, send_b, recv_t, recv_b, acc, st, sb, rt, rb):
    z, d = lax.axis_index("sky"), lax.axis_index("depth")
    me = z * depth + d
    devices = sky * depth
    visits, entries_rows, columns = tiles_ref.shape
    entries, rows, _ = warped.shape
    share = rows // depth

    def place(j):
        return lax.div(lax.rem(me + j, devices), depth), lax.rem(lax.rem(me + j, devices), depth)

    barrier = pltpu.get_barrier_semaphore()

    def greet(j, _):
        zz, dd = place(j)
        pl.semaphore_signal(barrier, inc=1, device_id={"sky": zz, "depth": dd}, device_id_type=MESH)
        return 0

    lax.fori_loop(1, devices, greet, 0)

    per_visit = entries // visits
    for v in range(visits):
        def warp(i, _, v=v):
            start = pl.multiple_of(i * STEP * rows, STEP * rows)
            product = jnp.dot(tiles_ref[v, pl.ds(start, STEP * rows), :], matrix_ref[v],
                              preferred_element_type=jnp.float32) * scale_ref[v]
            warped[pl.ds(v * per_visit + i * STEP, STEP)] = product.astype(jnp.bfloat16).reshape(STEP, rows, columns)
            return 0
        lax.fori_loop(0, per_visit // STEP, warp, 0)

    pl.semaphore_wait(barrier, devices - 1)

    def copies(zz, dd, there, mine):
        to = {"sky": zz, "depth": dd}
        return (
            pltpu.make_async_remote_copy(src_ref=send_t.at[there], dst_ref=recv_t.at[mine], send_sem=st.at[there],
                                         recv_sem=rt.at[mine], device_id=to, device_id_type=MESH),
            pltpu.make_async_remote_copy(src_ref=send_b.at[there], dst_ref=recv_b.at[mine], send_sem=sb.at[there],
                                         recv_sem=rb.at[mine], device_id=to, device_id_type=MESH),
        )

    def post(jj, _):
        zz = lax.rem(z + sky // 2 + jj, sky)

        def fill(s, _):
            e = src_ref[zz * SLOTS + s]
            valid = (e < entries).astype(jnp.int32)
            e = jnp.minimum(e, entries - 1)
            block = warped[e]
            flags = bits_ref[e] * valid
            for dd in range(depth):
                send_t[zz * depth + dd, s] = block[dd * share:(dd + 1) * share]
                send_b[zz * depth + dd, s] = flags[dd * (share // 16):(dd + 1) * (share // 16)]
            return 0

        lax.fori_loop(0, SLOTS, fill, 0)

        def start(k, _):
            dd = lax.rem(d + k, depth)
            there = zz * depth + dd

            @pl.when(there != me)
            def _():
                for c in copies(zz, dd, there, me):
                    c.start()
            return 0

        lax.fori_loop(0, depth, start, 0)
        return 0

    lax.fori_loop(0, sky, post, 0)

    acc[...] = jnp.zeros_like(acc)
    position = lax.rem(lax.broadcasted_iota(jnp.int32, (share, columns), 0), 16)

    def add(tiles, flags, source):
        for p in range(PATCH_DEV):
            sums = [acc[p, q] for q in range(6)]
            for c in range(CAPACITY):
                w = tiles[source, p * CAPACITY + c].astype(jnp.float32)
                packed = flags[source, p * CAPACITY + c]
                packed = jnp.broadcast_to(packed[:, None, :], (share // 16, 16, columns)).reshape(share, columns)
                shifted = lax.shift_right_logical(packed, position)
                first = (shifted & 1).astype(jnp.float32)
                both = first * (lax.shift_right_logical(shifted, 16) & 1).astype(jnp.float32)
                fw, bw = first * w, both * w
                for q, term in enumerate((first, fw, fw * w, both, bw, bw * w)):
                    sums[q] = sums[q] + term
            for q in range(6):
                acc[p, q] = sums[q]

    add(send_t, send_b, me)

    def take(jj, _):
        zz = lax.rem(z - sky // 2 - jj + 2 * sky, sky)

        def one(k, _):
            dd = lax.rem(d - k + depth, depth)
            there = zz * depth + dd

            @pl.when(there != me)
            def _():
                for c in copies(zz, dd, there, there):
                    c.wait_recv()
                add(recv_t, recv_b, there)
            return 0

        lax.fori_loop(0, depth, one, 0)
        return 0

    lax.fori_loop(0, sky, take, 0)

    for p in range(PATCH_DEV):
        cf, sf, qf, cb, sb_, qb = [acc[p, q] for q in range(6)]
        mean = sf / jnp.maximum(cf, 1.0)
        shift = sb_ - mean * cb
        square = qb - mean * sb_ - mean * shift
        step = shift / jnp.maximum(cb, 1.0)
        mean_ref[0, p] = mean
        mean_ref[1, p] = mean + step
        var_ref[0, p] = (qf - sf * mean) / jnp.maximum(cf - 1.0, 1.0)
        var_ref[1, p] = (square - shift * step) / jnp.maximum(cb - 1.0, 1.0)

    def drain(j, _):
        zz, dd = place(j)
        for c in copies(zz, dd, zz * depth + dd, me):
            c.wait_send()
        return 0

    lax.fori_loop(1, devices, drain, 0)


def folded(depth, scale_hbm, lists_hbm, tiles_hbm, matrix_hbm, bits_hbm, out_ref,
           scale_ref, lists_ref, tiles_ref, matrix_ref, bits_ref, s_in,
           out_t, out_b, row_t, row_b, raw_t, raw_b, own_s, held_s, far32, far16, got32, got16, tables, local, part,
           work_t, work_b, s_x, s_y, s_s, r_x, r_y, r_s, r_g, s_l):
    z, d = lax.axis_index("sky"), lax.axis_index("depth")
    half = z // 2
    rem = z - 2 * half
    inner, outer = rem != half, rem == half
    mate = 2 * half + 1 - rem
    across, beyond = 3 - z, 3 - mate
    base = d // 2 * 2
    other = depth - 2 - base
    twin = 2 * base + 1 - d
    parts, _, entries, slab, width = out_t.shape
    visits, entries_rows, columns = tiles_ref.shape
    per_visit = entries // visits
    rows = entries_rows // per_visit
    share = rows // depth
    slabs = share // slab
    long = own_s.shape[1]

    bands = matrix_ref.shape[0]
    first = bands // 2 * slabs + slabs - SWAP
    chain = parts - SWAP

    def chunk(i):
        return i + jnp.where(i >= first, SWAP, 0)

    def swapped(c):
        return jnp.logical_and(c >= first, c < first + SWAP)

    def fresh(c):
        return jnp.logical_or(c % slabs == 0, c == first)

    tiles_in = pltpu.make_async_copy(tiles_hbm, tiles_ref, s_in.at[bands])
    bits_in = pltpu.make_async_copy(bits_hbm, bits_ref, s_in.at[bands + 1])
    scale_in = pltpu.make_async_copy(scale_hbm, scale_ref, s_in.at[bands + 2])
    lists_in = pltpu.make_async_copy(lists_hbm, lists_ref, s_in.at[bands + 3])

    def matrix_in(band):
        lanes = pl.ds(band * width, width)
        return pltpu.make_async_copy(matrix_hbm.at[:, :, lanes], matrix_ref.at[band], s_in.at[band])

    barrier = pltpu.get_barrier_semaphore()
    for k in range(1, depth):
        pl.semaphore_signal(barrier, inc=1, device_id={"depth": lax.rem(d + k, depth)}, device_id_type=MESH)
    for k in range(depth):
        pl.semaphore_signal(barrier, inc=1, device_id={"sky": mate, "depth": k}, device_id_type=MESH)
    for far in (across, beyond):
        pl.semaphore_signal(barrier, inc=1, device_id={"sky": far}, device_id_type=MESH)

    tiles_in.start()
    matrix_in(0).start()
    lists_in.start()
    scale_in.start()
    bits_in.start()

    def remote(src, dst, send, recv, to):
        return pltpu.make_async_remote_copy(src_ref=src, dst_ref=dst, send_sem=send, recv_sem=recv, device_id=to,
                                            device_id_type=MESH)

    def to_row(c, there):
        return remote(out_t.at[c, there], row_t.at[c, d], s_x.at[0], r_x.at[c], {"depth": there})

    def flags_to_row(b, there):
        return remote(out_b.at[b, there], row_b.at[b, d], s_x.at[1], r_x.at[slabs * b], {"depth": there})

    def table_to_row(there):
        return remote(own_s, held_s.at[d], s_s.at[0], r_s.at[0], {"depth": there})

    def table_to_mates(there):
        return remote(own_s, held_s.at[depth + d], s_s.at[0], r_s.at[1], {"sky": mate, "depth": there})

    def direct(c, there):
        to = {"sky": mate, "depth": there}
        return remote(out_t.at[c, there], raw_t.at[c, d], s_y.at[0], r_y.at[c], to)

    def flags_direct(c, there):
        to = {"sky": mate, "depth": there}
        b = c // slabs
        return remote(out_b.at[b, there], raw_b.at[b, d], s_y.at[1], r_y.at[c], to)

    def onward(c):
        pair = pl.ds(other, 2)
        return remote(row_t.at[c, pair], raw_t.at[c, pair], s_y.at[0], r_y.at[c], {"sky": mate})

    def flags_onward(c):
        b, pair = c // slabs, pl.ds(other, 2)
        return remote(row_b.at[b, pair], raw_b.at[b, pair], s_y.at[1], r_y.at[c], {"sky": mate})

    def sums_to(c, t, where, slot):
        to = {"sky": where}
        return (remote(far32.at[c, t], got32.at[c, slot], s_y.at[2], r_g.at[c], to),
                remote(far16.at[c, t], got16.at[c, slot], s_y.at[3], r_g.at[c], to))

    def arrived(ref, sem):
        remote(ref, ref, s_x.at[0], sem, {"sky": mate}).wait_recv()

    def left(ref, sem):
        remote(ref, ref, sem, r_s.at[0], {"sky": mate}).wait_send()

    def volume(tiles):
        a, b, k = next((a, b, k) for a in range(1, parts + 1) for b in range(1, depth + 1)
                       for k in range(1, entries + 1) if a * b * k == tiles)
        return out_t.at[pl.ds(0, a), pl.ds(0, b), pl.ds(0, k)]

    def blocks_arrived(c, flags, sem, count):
        flag_tiles = 2 * entries // slab

        @pl.when(flags)
        def _():
            arrived(volume(count * (entries + flag_tiles)), sem.at[c])

        @pl.when(jnp.logical_not(flags))
        def _():
            arrived(volume(count * entries), sem.at[c])

    def row_arrived(c):
        blocks_arrived(c, c % slabs == 0, r_x, depth - 1)

    def raw_arrived(c):
        blocks_arrived(c, fresh(c), r_y, depth)

    def sums_arrived(c, slots):
        arrived(volume(slots * PATCH_DEV * 7), r_g.at[c])

    position = lax.broadcasted_iota(jnp.int32, (slab, width), 0)
    for which in range(2):
        for dd in range(depth):
            work_t[which, dd, entries] = jnp.zeros((slab, width), jnp.bfloat16)
            work_b[which, dd, entries] = jnp.zeros((1, width), jnp.int32)

    lists_in.wait()
    for band in range(1, bands):
        matrix_in(band).start()
    lane = lax.broadcasted_iota(jnp.int32, (1, long), 1)
    table = jnp.full((1, long), entries, jnp.int32)
    targets = [lists_ref[v, k] for v in range(visits) for k in range(per_visit)]
    for e in range(entries):
        rank = jnp.int32(0)
        for f in range(e // per_visit * per_visit):
            rank = rank + (targets[e] == targets[f]).astype(jnp.int32)
        table = jnp.where(lane == targets[e] * CAPACITY + rank, e, table)
    own_s[...] = table
    held_s[d] = table

    def stage(c, which, tiles, flags):
        work_t[which, :, :entries] = tiles[c]
        work_b[which, :, :entries] = flags[c // slabs]

    def gather(c, patch, groups, start=0):
        place = position + (c % slabs) * slab
        sums = [jnp.zeros((slab, width), jnp.float32)] * 6
        for which in range(start, groups):
            for dd in range(depth):
                for k in range(CAPACITY):
                    e = tables[which, dd, 0, patch * CAPACITY + k]
                    w = work_t[which, dd, e].astype(jnp.float32)
                    packed = jnp.broadcast_to(work_b[which, dd, e], (slab, width))
                    shifted = lax.shift_right_logical(packed, place)
                    first = (shifted & 1).astype(jnp.float32)
                    both = first * (lax.shift_right_logical(shifted, 16) & 1).astype(jnp.float32)
                    fw, bw = first * w, both * w
                    sums = [a + b for a, b in zip(sums, (first, fw, fw * w, both, bw, bw * w))]
        return sums

    def keep_part(c, t, where):
        def one(p, _):
            for q, value in enumerate(gather(c, where * PATCH_DEV + p, 1)):
                part[t, p, q] = value
            return 0
        lax.fori_loop(0, PATCH_DEV, one, 0)

    def send_sums(c, t, where, groups):
        def one(p, _):
            sums = gather(c, where * PATCH_DEV + p, groups, groups - 1)
            if groups == 2:
                sums = [part[t, p, q] + value for q, value in enumerate(sums)]
            cf, sf, qf, cb, sb, qb = sums
            mean = sf / jnp.maximum(cf, 1.0)
            far32[c, t, p] = sf
            packed = (cf, cb, qf - sf * mean, sb - mean * cb, qb - sb * (sb / jnp.maximum(cb, 1.0)))
            for q, value in enumerate(packed):
                far16[c, t, p, q] = value.astype(jnp.bfloat16)
            return 0
        lax.fori_loop(0, PATCH_DEV, one, 0)
        for copy in sums_to(c, t, where, half):
            copy.start()

    def send_all(c):
        for there in (other, other + 1, base, base + 1):
            flags_direct(c, there).start()
            direct(c, there).start()

    def send_direct(c):
        @pl.when(fresh(c))
        def _():
            for j in range(2):
                flags_direct(c, base + j).start()
        for j in range(2):
            direct(c, base + j).start()

    def send_onward(c):
        @pl.when(fresh(c))
        def _():
            flags_onward(c).start()
        onward(c).start()

    def warp(column, _):
        lanes = pl.ds(pl.multiple_of(column * width, width), width)
        for band in range(bands):
            @pl.when(column == band)
            def _(band=band):
                matrix_in(band).wait()
        for v in range(visits):
            product = jnp.dot(tiles_ref[v], matrix_ref[column, v], preferred_element_type=jnp.float32)
            block = (product * scale_ref[v]).reshape(per_visit, depth, slabs, slab, width)
            for dd in range(depth):
                for h in range(slabs):
                    out_t[column * slabs + h, dd, v * per_visit:(v + 1) * per_visit] = block[:, dd, h].astype(jnp.bfloat16)
        for dd in range(depth):
            out_b[column, dd] = bits_ref[:, dd:dd + 1, lanes]
        row_b[column, d] = out_b[column, d]
        for h in range(slabs):
            row_t[column * slabs + h, d] = out_t[column * slabs + h, d]

        @pl.when(column == 0)
        def _():
            pl.semaphore_wait(barrier, 2 * depth + 1)
            for k in range(1, depth):
                table_to_row(lax.rem(d + k, depth)).start()
            for k in range(depth):
                table_to_mates(k).start()

        late = jnp.logical_and(outer, column == 0)

        @pl.when(late)
        def _():
            send_all(0)

        def spread(h):
            for there in (other, other + 1, twin):
                if h == 0:
                    flags_to_row(column, there).start()
                to_row(column * slabs + h, there).start()

        for h in range(slabs):
            c = column * slabs + h
            if h == 0:
                @pl.when(jnp.logical_not(late))
                def _():
                    spread(0)
            else:
                spread(h)
            ahead = jnp.logical_and(outer, jnp.logical_and(c > 0, c < PRE))

            @pl.when(jnp.logical_or(ahead, jnp.logical_and(inner, swapped(c))))
            def _(c=c):
                send_direct(c)

        @pl.when(late)
        def _():
            spread(0)
        return 0

    tiles_in.wait()
    scale_in.wait()
    bits_in.wait()
    lax.fori_loop(0, bands, warp, 0)
    mine, theirs = (row_t, row_b), (raw_t, raw_b)

    def row_tables():
        arrived(held_s.at[pl.ds(0, depth - 1)], r_s.at[0])
        held = pltpu.make_async_copy(held_s.at[pl.ds(0, depth)], tables.at[0], s_l.at[0])
        held.start()
        return held

    def total(c, slot, p):
        sf = got32[c, slot, p]
        cf, cb, mf, shift, mb = [got16[c, slot, p, q].astype(jnp.float32) for q in range(5)]
        mean = sf / jnp.maximum(cf, 1.0)
        sb = shift + mean * cb
        return cf, sf, mf + sf * mean, cb, sb, mb + sb * (sb / jnp.maximum(cb, 1.0))

    def keep_local(c, groups):
        def one(p, _):
            for q, value in enumerate(gather(c, z * PATCH_DEV + p, groups)):
                local[c, p, q] = value
            return 0
        lax.fori_loop(0, PATCH_DEV, one, 0)

    def finish(c):
        lanes = pl.ds(pl.multiple_of(c // slabs * width, width), width)
        hub = jnp.logical_xor(inner, swapped(c))

        @pl.when(hub)
        def _():
            sums_arrived(c, 1)

        @pl.when(jnp.logical_not(hub))
        def _():
            sums_arrived(c, 2)
            for p in range(PATCH_DEV):
                for q, value in enumerate(total(c, half, p)):
                    local[c, p, q] = local[c, p, q] + value

        for p in range(PATCH_DEV):
            cf, sf, qf, cb, sb, qb = [local[c, p, q] + value for q, value in enumerate(total(c, 1 - half, p))]
            mean = sf / jnp.maximum(cf, 1.0)
            shift = sb - mean * cb
            square = qb - mean * sb - mean * shift
            step = shift / jnp.maximum(cb, 1.0)
            first_var = (qf - sf * mean) / jnp.maximum(cf - 1.0, 1.0)
            final_var = (square - shift * step) / jnp.maximum(cb - 1.0, 1.0)
            for h in range(slabs):
                @pl.when(c % slabs == h)
                def _(h=h, p=p, values=(mean, mean + step, first_var, final_var)):
                    for q, value in enumerate(values):
                        out_ref[q // 2, q % 2, p, h * slab:(h + 1) * slab, lanes] = value

    def all_tables():
        held = row_tables()
        arrived(held_s.at[pl.ds(0, depth)], r_s.at[1])
        more = pltpu.make_async_copy(held_s.at[pl.ds(depth, depth)], tables.at[1], s_l.at[1])
        more.start()
        held.wait()
        more.wait()

    @pl.when(outer)
    def _():
        def leaf(i, _):
            c = chunk(i)
            row_arrived(c)
            send_onward(c)

            @pl.when(i < LEAD - PRE)
            def _():
                send_direct(chunk(i + PRE))

            @pl.when(jnp.logical_and(i >= LEAD - 1, i + 1 < chain))
            def _():
                send_direct(chunk(i + 1))
            return 0

        lax.fori_loop(1, chain, leaf, 0)
        row_arrived(0)
        all_tables()

        def own(i, _):
            c = chunk(i)
            stage(c, 0, *mine)
            keep_local(c, 1)
            return 0

        lax.fori_loop(0, chain, own, 0)

        def turned(c, _):
            row_arrived(c)
            raw_arrived(c)
            stage(c, 0, *mine)
            keep_part(c, 0, beyond)
            keep_part(c, 1, across)
            stage(c, 1, *theirs)
            send_sums(c, 1, across, 2)
            send_sums(c, 0, beyond, 2)
            send_sums(c, 2, mate, 1)
            keep_local(c, 2)
            return 0

        lax.fori_loop(first, first + SWAP, turned, 0)

    @pl.when(inner)
    def _():
        all_tables()

        def hub(i, _):
            c = chunk(i)

            row_arrived(c)

            @pl.when(i == TURN)
            def _():
                def turned(q, _):
                    row_arrived(q)
                    send_onward(q)
                    stage(q, 0, *mine)
                    keep_local(q, 1)
                    return 0
                lax.fori_loop(first, first + SWAP, turned, 0)

            stage(c, 0, *mine)
            send_sums(c, 2, mate, 1)
            keep_part(c, 0, beyond)
            keep_part(c, 1, across)
            raw_arrived(c)
            stage(c, 1, *theirs)
            send_sums(c, 0, beyond, 2)
            send_sums(c, 1, across, 2)
            keep_local(c, 2)

            @pl.when(i >= LAG)
            def _():
                finish(chunk(i - LAG))
            return 0

        lax.fori_loop(0, chain, hub, 0)

    def close(i, _):
        @pl.when(jnp.logical_or(outer, i >= chain - LAG))
        def _():
            turn = jnp.logical_and(i >= chain - 1, i < parts - 1)
            finish(jnp.where(turn, i - chain + 1 + first, chunk(jnp.minimum(i, chain - 1))))
        return 0

    lax.fori_loop(0, parts, close, 0)

    left(out_t.at[:, pl.ds(0, depth - 1)], s_x.at[0])
    left(out_b.at[:, pl.ds(0, depth - 1)], s_x.at[1])

    left(held_s.at[pl.ds(0, 2 * depth - 1)], s_s.at[0])

    def all_left(sent, bands_sent, summed):
        left(out_t.at[pl.ds(0, sent)], s_y.at[0])
        left(out_b.at[pl.ds(0, bands_sent)], s_y.at[1])
        left(far32.at[pl.ds(0, summed)], s_y.at[2])
        left(far16.at[pl.ds(0, summed)], s_y.at[3])

    @pl.when(outer)
    def _():
        all_left(chain, bands, SWAP)

    @pl.when(inner)
    def _():
        all_left(SWAP, 1, chain)


def split(both_ref, mean_hbm, var_hbm, sems):
    outs = (mean_hbm, var_hbm)
    steps, patches = mean_hbm.shape[:2]
    pieces = PIECES // steps
    each = patches // pieces
    for t in range(steps):
        for p in range(pieces):
            part = pl.ds(p * each, each)
            for q, out in enumerate(outs):
                pltpu.make_async_copy(both_ref.at[q, t, part], out.at[t, part], sems.at[q]).start()
    for q, out in enumerate(outs):
        pltpu.make_async_copy(both_ref.at[q], out, sems.at[q]).wait()


def per_device(sky, depth, visit_tiles, warp_matrix, flux_scale, patch_lists, clip_bits):
    visits, own, rows, columns = visit_tiles.shape
    entries = visits * own
    patches = PATCH_DEV * sky
    devices = sky * depth
    share = rows // depth
    smem, vmem = pl.BlockSpec(memory_space=pltpu.SMEM), pl.BlockSpec(memory_space=pltpu.VMEM)
    hbm = pl.BlockSpec(memory_space=pltpu.HBM)
    out = jax.ShapeDtypeStruct((2, PATCH_DEV, share, columns), jnp.float32)
    if sky == 4 and depth == 4 and share == 16:
        width = 128
        slab = SLAB
        bands = columns // width
        parts = bands * (share // slab)
        long = -(-patches * CAPACITY // 128) * 128
        blocks = (parts, depth, entries, slab, width)
        flags = (bands, depth, entries, 1, width)
        work = (2, depth, entries + 1)
        dma = pltpu.SemaphoreType.DMA
        both = pl.pallas_call(
            functools.partial(folded, depth),
            out_shape=jax.ShapeDtypeStruct((2,) + out.shape, jnp.float32),
            in_specs=[hbm] * 5,
            out_specs=vmem,
            scratch_shapes=[
                pltpu.SMEM((visits,), jnp.float32),
                pltpu.SMEM((visits, own), jnp.int32),
                pltpu.VMEM((visits, own * rows, columns), jnp.bfloat16),
                pltpu.VMEM((bands, visits, columns, width), jnp.bfloat16),
                pltpu.VMEM((entries, rows // 16, columns), jnp.int32),
                dma((bands + 4,)),
                pltpu.VMEM(blocks, jnp.bfloat16), pltpu.VMEM(flags, jnp.int32),
                pltpu.VMEM(blocks, jnp.bfloat16), pltpu.VMEM(flags, jnp.int32),
                pltpu.VMEM(blocks, jnp.bfloat16), pltpu.VMEM(flags, jnp.int32),
                pltpu.VMEM((1, long), jnp.int32), pltpu.VMEM((2 * depth, 1, long), jnp.int32),
                pltpu.VMEM((parts, 3, PATCH_DEV, slab, width), jnp.float32),
                pltpu.VMEM((parts, 3, PATCH_DEV, 5, slab, width), jnp.bfloat16),
                pltpu.VMEM((parts, 2, PATCH_DEV, slab, width), jnp.float32),
                pltpu.VMEM((parts, 2, PATCH_DEV, 5, slab, width), jnp.bfloat16),
                pltpu.SMEM((2, depth, 1, long), jnp.int32),
                pltpu.VMEM((parts, PATCH_DEV, 6, slab, width), jnp.float32),
                pltpu.VMEM((2, PATCH_DEV, 6, slab, width), jnp.float32),
                pltpu.VMEM(work + blocks[3:], jnp.bfloat16), pltpu.VMEM(work + flags[3:], jnp.int32),
                dma((2,)), dma((4,)), dma((1,)), dma((parts,)), dma((parts,)), dma((2,)), dma((parts,)), dma((2,)),
            ],
            compiler_params=pltpu.CompilerParams(
                collective_id=0, has_side_effects=True, vmem_limit_bytes=24 * 1024 * 1024
            ),
        )(*[pltpu.with_memory_space_constraint(x, pltpu.HBM) for x in (
            flux_scale, patch_lists, visit_tiles.reshape(visits, own * rows, columns), warp_matrix,
            clip_bits.reshape(entries, rows // 16, columns))])
        return pl.pallas_call(
            split, out_shape=(out, out), in_specs=[vmem], out_specs=(hbm, hbm),
            scratch_shapes=[dma((2,))],
            compiler_params=pltpu.CompilerParams(vmem_limit_bytes=8 * 1024 * 1024),
        )(both)
    targets = patch_lists.reshape(entries)
    number = jnp.arange(entries, dtype=jnp.int32)
    same = (targets[:, None] == targets[None, :]) & (number[None, :] < number[:, None])
    rank = jnp.sum(same.astype(jnp.int32), axis=1)
    slot = targets * CAPACITY + rank
    source = jnp.min(
        jnp.where(slot[None, :] == jnp.arange(patches * CAPACITY, dtype=jnp.int32)[:, None], number[None, :], entries),
        axis=1,
    )
    return pl.pallas_call(
        functools.partial(kernel, sky, depth),
        out_shape=(out, out),
        in_specs=[smem, smem, vmem, vmem, vmem],
        out_specs=(vmem, vmem),
        scratch_shapes=[
            pltpu.VMEM((entries, rows, columns), jnp.bfloat16),
            pltpu.VMEM((devices, SLOTS, share, columns), jnp.bfloat16),
            pltpu.VMEM((devices, SLOTS, share // 16, columns), jnp.int32),
            pltpu.VMEM((devices, SLOTS, share, columns), jnp.bfloat16),
            pltpu.VMEM((devices, SLOTS, share // 16, columns), jnp.int32),
            pltpu.VMEM((PATCH_DEV, 6, share, columns), jnp.float32),
        ] + [pltpu.SemaphoreType.DMA((devices,))] * 4,
        compiler_params=pltpu.CompilerParams(
            collective_id=0, has_side_effects=True, vmem_limit_bytes=67043328 - 1048576
        ),
    )(flux_scale, source, visit_tiles.reshape(visits, own * rows, columns), warp_matrix,
      clip_bits.reshape(entries, rows // 16, columns))


def solution(mesh):
    whole = ("tracts", "sky", "depth")
    placed = (P(whole, None, None, None), P(whole, None, None), P(whole), P(whole, None), P(whole, None, None, None))
    outs = P(None, ("tracts", "sky"), "depth", None)
    return jax.shard_map(
        functools.partial(per_device, mesh.shape["sky"], mesh.shape["depth"]),
        mesh=mesh,
        in_specs=placed,
        out_specs=(outs, outs),
        check_vma=False,
    )
```

```python
import functools

import jax
import jax.numpy as jnp
from jax import lax
from jax.experimental import pallas as pl
from jax.experimental.pallas import tpu as pltpu
from jax.sharding import PartitionSpec as P

PATCH_DEV = 4
CAPACITY = 2
SLOTS = PATCH_DEV * CAPACITY
MESH = pl.DeviceIdType.MESH
STEP = 4
LAG = 5
LEAD = 6
PRE = 6
SLAB = 4
PIECES = 8
SWAP = 3
TURN = 8


def kernel(sky, depth, scale_ref, src_ref, tiles_ref, matrix_ref, bits_ref, mean_ref, var_ref,
           warped, send_t, send_b, recv_t, recv_b, acc, st, sb, rt, rb):
    z, d = lax.axis_index("sky"), lax.axis_index("depth")
    me = z * depth + d
    devices = sky * depth
    visits, entries_rows, columns = tiles_ref.shape
    entries, rows, _ = warped.shape
    share = rows // depth

    def place(j):
        return lax.div(lax.rem(me + j, devices), depth), lax.rem(lax.rem(me + j, devices), depth)

    barrier = pltpu.get_barrier_semaphore()

    def greet(j, _):
        zz, dd = place(j)
        pl.semaphore_signal(barrier, inc=1, device_id={"sky": zz, "depth": dd}, device_id_type=MESH)
        return 0

    lax.fori_loop(1, devices, greet, 0)

    per_visit = entries // visits
    for v in range(visits):
        def warp(i, _, v=v):
            start = pl.multiple_of(i * STEP * rows, STEP * rows)
            product = jnp.dot(tiles_ref[v, pl.ds(start, STEP * rows), :], matrix_ref[v],
                              preferred_element_type=jnp.float32) * scale_ref[v]
            warped[pl.ds(v * per_visit + i * STEP, STEP)] = product.astype(jnp.bfloat16).reshape(STEP, rows, columns)
            return 0
        lax.fori_loop(0, per_visit // STEP, warp, 0)

    pl.semaphore_wait(barrier, devices - 1)

    def copies(zz, dd, there, mine):
        to = {"sky": zz, "depth": dd}
        return (
            pltpu.make_async_remote_copy(src_ref=send_t.at[there], dst_ref=recv_t.at[mine], send_sem=st.at[there],
                                         recv_sem=rt.at[mine], device_id=to, device_id_type=MESH),
            pltpu.make_async_remote_copy(src_ref=send_b.at[there], dst_ref=recv_b.at[mine], send_sem=sb.at[there],
                                         recv_sem=rb.at[mine], device_id=to, device_id_type=MESH),
        )

    def post(jj, _):
        zz = lax.rem(z + sky // 2 + jj, sky)

        def fill(s, _):
            e = src_ref[zz * SLOTS + s]
            valid = (e < entries).astype(jnp.int32)
            e = jnp.minimum(e, entries - 1)
            block = warped[e]
            flags = bits_ref[e] * valid
            for dd in range(depth):
                send_t[zz * depth + dd, s] = block[dd * share:(dd + 1) * share]
                send_b[zz * depth + dd, s] = flags[dd * (share // 16):(dd + 1) * (share // 16)]
            return 0

        lax.fori_loop(0, SLOTS, fill, 0)

        def start(k, _):
            dd = lax.rem(d + k, depth)
            there = zz * depth + dd

            @pl.when(there != me)
            def _():
                for c in copies(zz, dd, there, me):
                    c.start()
            return 0

        lax.fori_loop(0, depth, start, 0)
        return 0

    lax.fori_loop(0, sky, post, 0)

    acc[...] = jnp.zeros_like(acc)
    position = lax.rem(lax.broadcasted_iota(jnp.int32, (share, columns), 0), 16)

    def add(tiles, flags, source):
        for p in range(PATCH_DEV):
            sums = [acc[p, q] for q in range(6)]
            for c in range(CAPACITY):
                w = tiles[source, p * CAPACITY + c].astype(jnp.float32)
                packed = flags[source, p * CAPACITY + c]
                packed = jnp.broadcast_to(packed[:, None, :], (share // 16, 16, columns)).reshape(share, columns)
                shifted = lax.shift_right_logical(packed, position)
                first = (shifted & 1).astype(jnp.float32)
                both = first * (lax.shift_right_logical(shifted, 16) & 1).astype(jnp.float32)
                fw, bw = first * w, both * w
                for q, term in enumerate((first, fw, fw * w, both, bw, bw * w)):
                    sums[q] = sums[q] + term
            for q in range(6):
                acc[p, q] = sums[q]

    add(send_t, send_b, me)

    def take(jj, _):
        zz = lax.rem(z - sky // 2 - jj + 2 * sky, sky)

        def one(k, _):
            dd = lax.rem(d - k + depth, depth)
            there = zz * depth + dd

            @pl.when(there != me)
            def _():
                for c in copies(zz, dd, there, there):
                    c.wait_recv()
                add(recv_t, recv_b, there)
            return 0

        lax.fori_loop(0, depth, one, 0)
        return 0

    lax.fori_loop(0, sky, take, 0)

    for p in range(PATCH_DEV):
        cf, sf, qf, cb, sb_, qb = [acc[p, q] for q in range(6)]
        mean = sf / jnp.maximum(cf, 1.0)
        shift = sb_ - mean * cb
        square = qb - mean * sb_ - mean * shift
        step = shift / jnp.maximum(cb, 1.0)
        mean_ref[0, p] = mean
        mean_ref[1, p] = mean + step
        var_ref[0, p] = (qf - sf * mean) / jnp.maximum(cf - 1.0, 1.0)
        var_ref[1, p] = (square - shift * step) / jnp.maximum(cb - 1.0, 1.0)

    def drain(j, _):
        zz, dd = place(j)
        for c in copies(zz, dd, zz * depth + dd, me):
            c.wait_send()
        return 0

    lax.fori_loop(1, devices, drain, 0)


def folded(depth, scale_hbm, lists_hbm, tiles_hbm, matrix_hbm, bits_hbm, out_ref,
           scale_ref, lists_ref, tiles_ref, matrix_ref, bits_ref, s_in,
           out_t, out_b, row_t, row_b, raw_t, raw_b, own_s, held_s, far32, far16, got32, got16, tables, local, part,
           work_t, work_b, s_x, s_y, s_s, r_x, r_y, r_s, r_g, s_l):
    z, d = lax.axis_index("sky"), lax.axis_index("depth")
    half = z // 2
    rem = z - 2 * half
    inner, outer = rem != half, rem == half
    mate = 2 * half + 1 - rem
    across, beyond = 3 - z, 3 - mate
    base = d // 2 * 2
    other = depth - 2 - base
    twin = 2 * base + 1 - d
    parts, _, entries, slab, width = out_t.shape
    visits, entries_rows, columns = tiles_ref.shape
    per_visit = entries // visits
    rows = entries_rows // per_visit
    share = rows // depth
    slabs = share // slab
    long = own_s.shape[1]

    bands = matrix_ref.shape[0]
    first = bands // 2 * slabs + slabs - SWAP
    chain = parts - SWAP

    def chunk(i):
        return i + jnp.where(i >= first, SWAP, 0)

    def swapped(c):
        return jnp.logical_and(c >= first, c < first + SWAP)

    def fresh(c):
        return jnp.logical_or(c % slabs == 0, c == first)

    tiles_in = pltpu.make_async_copy(tiles_hbm, tiles_ref, s_in.at[bands])
    bits_in = pltpu.make_async_copy(bits_hbm, bits_ref, s_in.at[bands + 1])
    scale_in = pltpu.make_async_copy(scale_hbm, scale_ref, s_in.at[bands + 2])
    lists_in = pltpu.make_async_copy(lists_hbm, lists_ref, s_in.at[bands + 3])

    def matrix_in(band):
        lanes = pl.ds(band * width, width)
        return pltpu.make_async_copy(matrix_hbm.at[:, :, lanes], matrix_ref.at[band], s_in.at[band])

    barrier = pltpu.get_barrier_semaphore()
    for k in range(1, depth):
        pl.semaphore_signal(barrier, inc=1, device_id={"depth": lax.rem(d + k, depth)}, device_id_type=MESH)
    for k in range(depth):
        pl.semaphore_signal(barrier, inc=1, device_id={"sky": mate, "depth": k}, device_id_type=MESH)
    for far in (across, beyond):
        pl.semaphore_signal(barrier, inc=1, device_id={"sky": far}, device_id_type=MESH)

    tiles_in.start()
    matrix_in(0).start()
    lists_in.start()
    scale_in.start()
    bits_in.start()

    def remote(src, dst, send, recv, to):
        return pltpu.make_async_remote_copy(src_ref=src, dst_ref=dst, send_sem=send, recv_sem=recv, device_id=to,
                                            device_id_type=MESH)

    def to_row(c, there):
        return remote(out_t.at[c, there], row_t.at[c, d], s_x.at[0], r_x.at[c], {"depth": there})

    def flags_to_row(b, there):
        return remote(out_b.at[b, there], row_b.at[b, d], s_x.at[1], r_x.at[slabs * b], {"depth": there})

    def table_to_row(there):
        return remote(own_s, held_s.at[d], s_s.at[0], r_s.at[0], {"depth": there})

    def table_to_mates(there):
        return remote(own_s, held_s.at[depth + d], s_s.at[0], r_s.at[1], {"sky": mate, "depth": there})

    def direct(c, there):
        to = {"sky": mate, "depth": there}
        return remote(out_t.at[c, there], raw_t.at[c, d], s_y.at[0], r_y.at[c], to)

    def flags_direct(c, there):
        to = {"sky": mate, "depth": there}
        b = c // slabs
        return remote(out_b.at[b, there], raw_b.at[b, d], s_y.at[1], r_y.at[c], to)

    def onward(c):
        pair = pl.ds(other, 2)
        return remote(row_t.at[c, pair], raw_t.at[c, pair], s_y.at[0], r_y.at[c], {"sky": mate})

    def flags_onward(c):
        b, pair = c // slabs, pl.ds(other, 2)
        return remote(row_b.at[b, pair], raw_b.at[b, pair], s_y.at[1], r_y.at[c], {"sky": mate})

    def sums_to(c, t, where, slot):
        to = {"sky": where}
        return (remote(far32.at[c, t], got32.at[c, slot], s_y.at[2], r_g.at[c], to),
                remote(far16.at[c, t], got16.at[c, slot], s_y.at[3], r_g.at[c], to))

    def arrived(ref, sem):
        remote(ref, ref, s_x.at[0], sem, {"sky": mate}).wait_recv()

    def left(ref, sem):
        remote(ref, ref, sem, r_s.at[0], {"sky": mate}).wait_send()

    def volume(tiles):
        a, b, k = next((a, b, k) for a in range(1, parts + 1) for b in range(1, depth + 1)
                       for k in range(1, entries + 1) if a * b * k == tiles)
        return out_t.at[pl.ds(0, a), pl.ds(0, b), pl.ds(0, k)]

    def blocks_arrived(c, flags, sem, count):
        flag_tiles = 2 * entries // slab

        @pl.when(flags)
        def _():
            arrived(volume(count * (entries + flag_tiles)), sem.at[c])

        @pl.when(jnp.logical_not(flags))
        def _():
            arrived(volume(count * entries), sem.at[c])

    def row_arrived(c):
        blocks_arrived(c, c % slabs == 0, r_x, depth - 1)

    def raw_arrived(c):
        blocks_arrived(c, fresh(c), r_y, depth)

    def sums_arrived(c, slots):
        arrived(volume(slots * PATCH_DEV * 7), r_g.at[c])

    position = lax.broadcasted_iota(jnp.int32, (slab, width), 0)
    for which in range(2):
        for dd in range(depth):
            work_t[which, dd, entries] = jnp.zeros((slab, width), jnp.bfloat16)
            work_b[which, dd, entries] = jnp.zeros((1, width), jnp.int32)

    lists_in.wait()
    for band in range(1, bands):
        matrix_in(band).start()
    lane = lax.broadcasted_iota(jnp.int32, (1, long), 1)
    table = jnp.full((1, long), entries, jnp.int32)
    targets = [lists_ref[v, k] for v in range(visits) for k in range(per_visit)]
    for e in range(entries):
        rank = jnp.int32(0)
        for f in range(e // per_visit * per_visit):
            rank = rank + (targets[e] == targets[f]).astype(jnp.int32)
        table = jnp.where(lane == targets[e] * CAPACITY + rank, e, table)
    own_s[...] = table
    held_s[d] = table

    def stage(c, which, tiles, flags):
        work_t[which, :, :entries] = tiles[c]
        work_b[which, :, :entries] = flags[c // slabs]

    def gather(c, patch, groups, start=0):
        place = position + (c % slabs) * slab
        sums = [jnp.zeros((slab, width), jnp.float32)] * 6
        for which in range(start, groups):
            for dd in range(depth):
                for k in range(CAPACITY):
                    e = tables[which, dd, 0, patch * CAPACITY + k]
                    w = work_t[which, dd, e].astype(jnp.float32)
                    packed = jnp.broadcast_to(work_b[which, dd, e], (slab, width))
                    shifted = lax.shift_right_logical(packed, place)
                    first = (shifted & 1).astype(jnp.float32)
                    both = first * (lax.shift_right_logical(shifted, 16) & 1).astype(jnp.float32)
                    fw, bw = first * w, both * w
                    sums = [a + b for a, b in zip(sums, (first, fw, fw * w, both, bw, bw * w))]
        return sums

    def keep_part(c, t, where):
        def one(p, _):
            for q, value in enumerate(gather(c, where * PATCH_DEV + p, 1)):
                part[t, p, q] = value
            return 0
        lax.fori_loop(0, PATCH_DEV, one, 0)

    def send_sums(c, t, where, groups):
        def one(p, _):
            sums = gather(c, where * PATCH_DEV + p, groups, groups - 1)
            if groups == 2:
                sums = [part[t, p, q] + value for q, value in enumerate(sums)]
            cf, sf, qf, cb, sb, qb = sums
            mean = sf / jnp.maximum(cf, 1.0)
            far32[c, t, p] = sf
            packed = (cf, cb, qf - sf * mean, sb - mean * cb, qb - sb * (sb / jnp.maximum(cb, 1.0)))
            for q, value in enumerate(packed):
                far16[c, t, p, q] = value.astype(jnp.bfloat16)
            return 0
        lax.fori_loop(0, PATCH_DEV, one, 0)
        for copy in sums_to(c, t, where, half):
            copy.start()

    def send_all(c):
        for there in (other, other + 1, base, base + 1):
            flags_direct(c, there).start()
            direct(c, there).start()

    def send_direct(c):
        @pl.when(fresh(c))
        def _():
            for j in range(2):
                flags_direct(c, base + j).start()
        for j in range(2):
            direct(c, base + j).start()

    def send_onward(c):
        @pl.when(fresh(c))
        def _():
            flags_onward(c).start()
        onward(c).start()

    def warp(column, _):
        lanes = pl.ds(pl.multiple_of(column * width, width), width)
        for band in range(bands):
            @pl.when(column == band)
            def _(band=band):
                matrix_in(band).wait()
        for v in range(visits):
            product = jnp.dot(tiles_ref[v], matrix_ref[column, v], preferred_element_type=jnp.float32)
            block = (product * scale_ref[v]).reshape(per_visit, depth, slabs, slab, width)
            for dd in range(depth):
                for h in range(slabs):
                    out_t[column * slabs + h, dd, v * per_visit:(v + 1) * per_visit] = block[:, dd, h].astype(jnp.bfloat16)
        for dd in range(depth):
            out_b[column, dd] = bits_ref[:, dd:dd + 1, lanes]
        row_b[column, d] = out_b[column, d]
        for h in range(slabs):
            row_t[column * slabs + h, d] = out_t[column * slabs + h, d]

        @pl.when(column == 0)
        def _():
            pl.semaphore_wait(barrier, 2 * depth + 1)
            for k in range(1, depth):
                table_to_row(lax.rem(d + k, depth)).start()
            for k in range(depth):
                table_to_mates(k).start()

        late = jnp.logical_and(outer, column == 0)

        @pl.when(late)
        def _():
            send_all(0)

        def spread(h):
            for there in (other, other + 1, twin):
                if h == 0:
                    flags_to_row(column, there).start()
                to_row(column * slabs + h, there).start()

        for h in range(slabs):
            c = column * slabs + h
            if h == 0:
                @pl.when(jnp.logical_not(late))
                def _():
                    spread(0)
            else:
                spread(h)
            ahead = jnp.logical_and(outer, jnp.logical_and(c > 0, c < PRE))

            @pl.when(jnp.logical_or(ahead, jnp.logical_and(inner, swapped(c))))
            def _(c=c):
                send_direct(c)

        @pl.when(late)
        def _():
            spread(0)
        return 0

    tiles_in.wait()
    scale_in.wait()
    bits_in.wait()
    lax.fori_loop(0, bands, warp, 0)
    mine, theirs = (row_t, row_b), (raw_t, raw_b)

    def row_tables():
        arrived(held_s.at[pl.ds(0, depth - 1)], r_s.at[0])
        held = pltpu.make_async_copy(held_s.at[pl.ds(0, depth)], tables.at[0], s_l.at[0])
        held.start()
        return held

    def total(c, slot, p):
        sf = got32[c, slot, p]
        cf, cb, mf, shift, mb = [got16[c, slot, p, q].astype(jnp.float32) for q in range(5)]
        mean = sf / jnp.maximum(cf, 1.0)
        sb = shift + mean * cb
        return cf, sf, mf + sf * mean, cb, sb, mb + sb * (sb / jnp.maximum(cb, 1.0))

    def keep_local(c, groups):
        def one(p, _):
            for q, value in enumerate(gather(c, z * PATCH_DEV + p, groups)):
                local[c, p, q] = value
            return 0
        lax.fori_loop(0, PATCH_DEV, one, 0)

    def finish(c):
        lanes = pl.ds(pl.multiple_of(c // slabs * width, width), width)
        hub = jnp.logical_xor(inner, swapped(c))

        @pl.when(hub)
        def _():
            sums_arrived(c, 1)

        @pl.when(jnp.logical_not(hub))
        def _():
            sums_arrived(c, 2)
            for p in range(PATCH_DEV):
                for q, value in enumerate(total(c, half, p)):
                    local[c, p, q] = local[c, p, q] + value

        for p in range(PATCH_DEV):
            cf, sf, qf, cb, sb, qb = [local[c, p, q] + value for q, value in enumerate(total(c, 1 - half, p))]
            mean = sf / jnp.maximum(cf, 1.0)
            shift = sb - mean * cb
            square = qb - mean * sb - mean * shift
            step = shift / jnp.maximum(cb, 1.0)
            first_var = (qf - sf * mean) / jnp.maximum(cf - 1.0, 1.0)
            final_var = (square - shift * step) / jnp.maximum(cb - 1.0, 1.0)
            for h in range(slabs):
                @pl.when(c % slabs == h)
                def _(h=h, p=p, values=(mean, mean + step, first_var, final_var)):
                    for q, value in enumerate(values):
                        out_ref[q // 2, q % 2, p, h * slab:(h + 1) * slab, lanes] = value

    def all_tables():
        held = row_tables()
        arrived(held_s.at[pl.ds(0, depth)], r_s.at[1])
        more = pltpu.make_async_copy(held_s.at[pl.ds(depth, depth)], tables.at[1], s_l.at[1])
        more.start()
        held.wait()
        more.wait()

    @pl.when(outer)
    def _():
        def leaf(i, _):
            c = chunk(i)
            row_arrived(c)
            send_onward(c)

            @pl.when(i < LEAD - PRE)
            def _():
                send_direct(chunk(i + PRE))

            @pl.when(jnp.logical_and(i >= LEAD - 1, i + 1 < chain))
            def _():
                send_direct(chunk(i + 1))
            return 0

        lax.fori_loop(1, chain, leaf, 0)
        row_arrived(0)
        all_tables()

        def own(i, _):
            c = chunk(i)
            stage(c, 0, *mine)
            keep_local(c, 1)
            return 0

        lax.fori_loop(0, chain, own, 0)

        def turned(c, _):
            row_arrived(c)
            raw_arrived(c)
            stage(c, 0, *mine)
            keep_part(c, 0, beyond)
            keep_part(c, 1, across)
            stage(c, 1, *theirs)
            send_sums(c, 1, across, 2)
            send_sums(c, 0, beyond, 2)
            send_sums(c, 2, mate, 1)
            keep_local(c, 2)
            return 0

        lax.fori_loop(first, first + SWAP, turned, 0)

    @pl.when(inner)
    def _():
        all_tables()

        def hub(i, _):
            c = chunk(i)

            row_arrived(c)

            @pl.when(i == TURN)
            def _():
                def turned(q, _):
                    row_arrived(q)
                    send_onward(q)
                    stage(q, 0, *mine)
                    keep_local(q, 1)
                    return 0
                lax.fori_loop(first, first + SWAP, turned, 0)

            stage(c, 0, *mine)
            send_sums(c, 2, mate, 1)
            keep_part(c, 0, beyond)
            keep_part(c, 1, across)
            raw_arrived(c)
            stage(c, 1, *theirs)
            send_sums(c, 0, beyond, 2)
            send_sums(c, 1, across, 2)
            keep_local(c, 2)

            @pl.when(i >= LAG)
            def _():
                finish(chunk(i - LAG))
            return 0

        lax.fori_loop(0, chain, hub, 0)

    def close(i, _):
        @pl.when(jnp.logical_or(outer, i >= chain - LAG))
        def _():
            turn = jnp.logical_and(i >= chain - 1, i < parts - 1)
            finish(jnp.where(turn, i - chain + 1 + first, chunk(jnp.minimum(i, chain - 1))))
        return 0

    lax.fori_loop(0, parts, close, 0)

    left(out_t.at[:, pl.ds(0, depth - 1)], s_x.at[0])
    left(out_b.at[:, pl.ds(0, depth - 1)], s_x.at[1])

    left(held_s.at[pl.ds(0, 2 * depth - 1)], s_s.at[0])

    def all_left(sent, bands_sent, summed):
        left(out_t.at[pl.ds(0, sent)], s_y.at[0])
        left(out_b.at[pl.ds(0, bands_sent)], s_y.at[1])
        left(far32.at[pl.ds(0, summed)], s_y.at[2])
        left(far16.at[pl.ds(0, summed)], s_y.at[3])

    @pl.when(outer)
    def _():
        all_left(chain, bands, SWAP)

    @pl.when(inner)
    def _():
        all_left(SWAP, 1, chain)


def split(both_ref, mean_hbm, var_hbm, sems):
    outs = (mean_hbm, var_hbm)
    steps, patches = mean_hbm.shape[:2]
    pieces = PIECES // steps
    each = patches // pieces
    for t in range(steps):
        for p in range(pieces):
            part = pl.ds(p * each, each)
            for q, out in enumerate(outs):
                pltpu.make_async_copy(both_ref.at[q, t, part], out.at[t, part], sems.at[q]).start()
    for q, out in enumerate(outs):
        pltpu.make_async_copy(both_ref.at[q], out, sems.at[q]).wait()


def per_device(sky, depth, visit_tiles, warp_matrix, flux_scale, patch_lists, clip_bits):
    visits, own, rows, columns = visit_tiles.shape
    entries = visits * own
    patches = PATCH_DEV * sky
    devices = sky * depth
    share = rows // depth
    smem, vmem = pl.BlockSpec(memory_space=pltpu.SMEM), pl.BlockSpec(memory_space=pltpu.VMEM)
    hbm = pl.BlockSpec(memory_space=pltpu.HBM)
    out = jax.ShapeDtypeStruct((2, PATCH_DEV, share, columns), jnp.float32)
    if sky == 4 and depth == 4 and share == 16:
        width = 128
        slab = SLAB
        bands = columns // width
        parts = bands * (share // slab)
        long = -(-patches * CAPACITY // 128) * 128
        blocks = (parts, depth, entries, slab, width)
        flags = (bands, depth, entries, 1, width)
        work = (2, depth, entries + 1)
        dma = pltpu.SemaphoreType.DMA
        both = pl.pallas_call(
            functools.partial(folded, depth),
            out_shape=jax.ShapeDtypeStruct((2,) + out.shape, jnp.float32),
            in_specs=[hbm] * 5,
            out_specs=vmem,
            scratch_shapes=[
                pltpu.SMEM((visits,), jnp.float32),
                pltpu.SMEM((visits, own), jnp.int32),
                pltpu.VMEM((visits, own * rows, columns), jnp.bfloat16),
                pltpu.VMEM((bands, visits, columns, width), jnp.bfloat16),
                pltpu.VMEM((entries, rows // 16, columns), jnp.int32),
                dma((bands + 4,)),
                pltpu.VMEM(blocks, jnp.bfloat16), pltpu.VMEM(flags, jnp.int32),
                pltpu.VMEM(blocks, jnp.bfloat16), pltpu.VMEM(flags, jnp.int32),
                pltpu.VMEM(blocks, jnp.bfloat16), pltpu.VMEM(flags, jnp.int32),
                pltpu.VMEM((1, long), jnp.int32), pltpu.VMEM((2 * depth, 1, long), jnp.int32),
                pltpu.VMEM((parts, 3, PATCH_DEV, slab, width), jnp.float32),
                pltpu.VMEM((parts, 3, PATCH_DEV, 5, slab, width), jnp.bfloat16),
                pltpu.VMEM((parts, 2, PATCH_DEV, slab, width), jnp.float32),
                pltpu.VMEM((parts, 2, PATCH_DEV, 5, slab, width), jnp.bfloat16),
                pltpu.SMEM((2, depth, 1, long), jnp.int32),
                pltpu.VMEM((parts, PATCH_DEV, 6, slab, width), jnp.float32),
                pltpu.VMEM((2, PATCH_DEV, 6, slab, width), jnp.float32),
                pltpu.VMEM(work + blocks[3:], jnp.bfloat16), pltpu.VMEM(work + flags[3:], jnp.int32),
                dma((2,)), dma((4,)), dma((1,)), dma((parts,)), dma((parts,)), dma((2,)), dma((parts,)), dma((2,)),
            ],
            compiler_params=pltpu.CompilerParams(
                collective_id=0, has_side_effects=True, vmem_limit_bytes=24 * 1024 * 1024
            ),
        )(*[pltpu.with_memory_space_constraint(x, pltpu.HBM) for x in (
            flux_scale, patch_lists, visit_tiles.reshape(visits, own * rows, columns), warp_matrix,
            clip_bits.reshape(entries, rows // 16, columns))])
        return pl.pallas_call(
            split, out_shape=(out, out), in_specs=[vmem], out_specs=(hbm, hbm),
            scratch_shapes=[dma((2,))],
            compiler_params=pltpu.CompilerParams(vmem_limit_bytes=8 * 1024 * 1024),
        )(both)
    targets = patch_lists.reshape(entries)
    number = jnp.arange(entries, dtype=jnp.int32)
    same = (targets[:, None] == targets[None, :]) & (number[None, :] < number[:, None])
    rank = jnp.sum(same.astype(jnp.int32), axis=1)
    slot = targets * CAPACITY + rank
    source = jnp.min(
        jnp.where(slot[None, :] == jnp.arange(patches * CAPACITY, dtype=jnp.int32)[:, None], number[None, :], entries),
        axis=1,
    )
    return pl.pallas_call(
        functools.partial(kernel, sky, depth),
        out_shape=(out, out),
        in_specs=[smem, smem, vmem, vmem, vmem],
        out_specs=(vmem, vmem),
        scratch_shapes=[
            pltpu.VMEM((entries, rows, columns), jnp.bfloat16),
            pltpu.VMEM((devices, SLOTS, share, columns), jnp.bfloat16),
            pltpu.VMEM((devices, SLOTS, share // 16, columns), jnp.int32),
            pltpu.VMEM((devices, SLOTS, share, columns), jnp.bfloat16),
            pltpu.VMEM((devices, SLOTS, share // 16, columns), jnp.int32),
            pltpu.VMEM((PATCH_DEV, 6, share, columns), jnp.float32),
        ] + [pltpu.SemaphoreType.DMA((devices,))] * 4,
        compiler_params=pltpu.CompilerParams(
            collective_id=0, has_side_effects=True, vmem_limit_bytes=67043328 - 1048576
        ),
    )(flux_scale, source, visit_tiles.reshape(visits, own * rows, columns), warp_matrix,
      clip_bits.reshape(entries, rows // 16, columns))


def solution(mesh):
    whole = ("tracts", "sky", "depth")
    placed = (P(whole, None, None, None), P(whole, None, None), P(whole), P(whole, None), P(whole, None, None, None))
    outs = P(None, ("tracts", "sky"), "depth", None)
    return jax.shard_map(
        functools.partial(per_device, mesh.shape["sky"], mesh.shape["depth"]),
        mesh=mesh,
        in_specs=placed,
        out_specs=(outs, outs),
        check_vma=False,
    )
```
